32 devices in a mesh: dp: 1 (over z), ep: 32 (over y, x, core).
Axes of the slice: x: 4, y: 4, z: 1, core: 2. Of those that a mesh axis runs over, the one named last changes fastest.
The devices are a block of a 4x4x8 slice.
Arguments:
- tokens: bfloat16 [12288, 1024], P(('dp', 'ep'))
- expert_ids: int32 [12288, 8], P(('dp', 'ep'))
- gate_vals: float32 [12288, 8], P(('dp', 'ep'))
- w_gate: bfloat16 [32, 1024, 512], P('ep')
- w_up: bfloat16 [32, 1024, 512], P('ep')
- w_down: bfloat16 [32, 512, 1024], P('ep')
- grad_out: bfloat16 [12288, 1024], P(('dp', 'ep'))
Outputs:
- output 1: bfloat16 [12288, 1024], P(('dp', 'ep'))
- output 2: bfloat16 [12288, 1024], P(('dp', 'ep'))
- output 3: bfloat16 [32, 1024, 512], P(('dp', 'ep'))
- output 4: bfloat16 [32, 1024, 512], P(('dp', 'ep'))
- output 5: bfloat16 [32, 512, 1024], P(('dp', 'ep'))
All inputs are finite; a program needn't handle non-finite values.
Results may differ from the reference program's by a relative error of at most 0.00104.
Values are sent between devices in bfloat16 or wider.
A program may use at most 768 MiB of HBM per device.

```python
import jax
import jax.numpy as jnp
from jax import lax

EP = 32
TOK = 384
D = 1024
FF = 512
EXPERTS = 32
TOP = 8

CAP = ((2 * TOK * TOP + 8 * EXPERTS - 1) // (8 * EXPERTS)) * 8
HOT = EXPERTS // 2


def chip_routing(chip_key, hot_count):
    sub_keys = jax.random.split(chip_key, 3)
    cold_order = jax.random.permutation(sub_keys[0], EXPERTS - 1)
    cold_ids = jnp.where(cold_order >= HOT, cold_order + 1, cold_order).astype(jnp.int32)
    rest_count = TOK * TOP - hot_count - CAP
    base_count = rest_count // (EXPERTS - 2)
    extra_count = rest_count % (EXPERTS - 2)
    cold_rank = jnp.arange(EXPERTS - 1)
    cold_count = jnp.where(cold_rank == 0, CAP, base_count + (cold_rank - 1 < extra_count).astype(jnp.int32))
    counts = jnp.concatenate([jnp.reshape(hot_count, (1,)), cold_count]).astype(jnp.int32)
    listed_ids = jnp.concatenate([jnp.full((1,), HOT, jnp.int32), cold_ids])
    count_ends = jnp.cumsum(counts)
    list_slot = jnp.searchsorted(count_ends, jnp.arange(TOK * TOP), side="right")
    id_grid = listed_ids[list_slot].reshape(TOP, TOK).T
    id_grid = id_grid[jax.random.permutation(sub_keys[1], TOK)]
    row_shift = jax.random.randint(sub_keys[2], (TOK, 1), 0, TOP)
    col_index = (jnp.arange(TOP)[None, :] + row_shift) % TOP
    return jnp.take_along_axis(id_grid, col_index, axis=1)


def draw_routing(route_key):
    sub_keys = jax.random.split(route_key, 3)
    full_chip = jax.random.randint(sub_keys[0], (), 0, EP)
    hot_count = jax.random.randint(sub_keys[1], (EP,), TOK // 4, TOK + 1)
    hot_count = jnp.where(jnp.arange(EP) == full_chip, TOK, hot_count).astype(jnp.int32)
    chip_ids = jax.vmap(chip_routing)(jax.random.split(sub_keys[2], EP), hot_count)
    return chip_ids.reshape(EP * TOK, TOP).astype(jnp.int32)


def setup_inputs(seed: int = 0, part: int = 0) -> dict:
    part_keys = jax.random.split(jax.random.fold_in(jax.random.key(seed), part), 4)
    weight_keys = jax.random.split(jax.random.key(seed + 1), 3)
    tokens = jax.random.normal(part_keys[0], (EP * TOK, D), jnp.float32).astype(jnp.bfloat16)
    expert_ids = draw_routing(part_keys[1])
    gate_vals = jax.random.uniform(part_keys[2], (EP * TOK, TOP), jnp.float32, 0.5, 1.5) * TOP ** -0.5
    w_gate = (jax.random.normal(weight_keys[0], (EXPERTS, D, FF), jnp.float32) * D ** -0.5).astype(jnp.bfloat16)
    w_up = (jax.random.normal(weight_keys[1], (EXPERTS, D, FF), jnp.float32) * D ** -0.5).astype(jnp.bfloat16)
    w_down = (jax.random.normal(weight_keys[2], (EXPERTS, FF, D), jnp.float32) * FF ** -0.5).astype(jnp.bfloat16)
    grad_out = jax.random.normal(part_keys[3], (EP * TOK, D), jnp.float32).astype(jnp.bfloat16)
    return {"tokens": tokens, "expert_ids": expert_ids, "gate_vals": gate_vals, "w_gate": w_gate, "w_up": w_up, "w_down": w_down, "grad_out": grad_out}


def expert_step(in_rows, d_rows_out, gate_w, up_w, down_w):
    act_a = jnp.dot(in_rows, gate_w, preferred_element_type=jnp.float32)
    act_b = jnp.dot(in_rows, up_w, preferred_element_type=jnp.float32)
    sig_a = jax.nn.sigmoid(act_a)
    hidden = (act_a * sig_a * act_b).astype(jnp.bfloat16)
    expert_out = jnp.dot(hidden, down_w, preferred_element_type=jnp.float32).astype(jnp.bfloat16)
    d_hidden = jnp.dot(d_rows_out, down_w.T, preferred_element_type=jnp.float32)
    d_act_a = (d_hidden * act_b * sig_a * (1.0 + act_a * (1.0 - sig_a))).astype(jnp.bfloat16)
    d_act_b = (d_hidden * act_a * sig_a).astype(jnp.bfloat16)
    d_rows = (jnp.dot(d_act_a, gate_w.T, preferred_element_type=jnp.float32) + jnp.dot(d_act_b, up_w.T, preferred_element_type=jnp.float32)).astype(jnp.bfloat16)
    grad_gate = jnp.dot(in_rows.T, d_act_a, preferred_element_type=jnp.float32)
    grad_up = jnp.dot(in_rows.T, d_act_b, preferred_element_type=jnp.float32)
    grad_down = jnp.dot(hidden.T, d_rows_out, preferred_element_type=jnp.float32)
    return expert_out, d_rows, grad_gate, grad_up, grad_down


def reference(tokens, expert_ids, gate_vals, w_gate, w_up, w_down, grad_out):
    num_rows = EP * TOK * TOP
    cold_cap = EP * CAP
    cold_total = EXPERTS * cold_cap
    flat_ids = expert_ids.reshape(num_rows)
    sort_order = jnp.argsort(flat_ids, stable=True)
    sorted_ids = flat_ids[sort_order]
    group_start = jnp.searchsorted(sorted_ids, jnp.arange(EXPERTS), side="left")
    sorted_rank = (jnp.arange(num_rows) - group_start[sorted_ids]).astype(jnp.int32)
    slot_rank = jnp.zeros((num_rows,), jnp.int32).at[sort_order].set(sorted_rank)
    buf_pos = jnp.where(flat_ids == HOT, cold_total + slot_rank, flat_ids * cold_cap + slot_rank)
    tok_rep = jnp.broadcast_to(tokens[:, None, :], (EP * TOK, TOP, D)).reshape(num_rows, D)
    d_rep = (gate_vals[:, :, None] * grad_out[:, None, :].astype(jnp.float32)).astype(jnp.bfloat16).reshape(num_rows, D)
    buf_rows = cold_total + EP * TOK
    x_buf = jnp.zeros((buf_rows, D), jnp.bfloat16).at[buf_pos].set(tok_rep)
    d_buf = jnp.zeros((buf_rows, D), jnp.bfloat16).at[buf_pos].set(d_rep)

    def cold_body(expert_in):
        return expert_step(expert_in[0], expert_in[1], expert_in[2], expert_in[3], expert_in[4])

    cold_res = lax.map(cold_body, (x_buf[:cold_total].reshape(EXPERTS, cold_cap, D), d_buf[:cold_total].reshape(EXPERTS, cold_cap, D), w_gate, w_up, w_down))
    hot_res = expert_step(x_buf[cold_total:], d_buf[cold_total:], w_gate[HOT], w_up[HOT], w_down[HOT])
    out_buf = jnp.concatenate([cold_res[0].reshape(cold_total, D), hot_res[0]], axis=0)
    dx_buf = jnp.concatenate([cold_res[1].reshape(cold_total, D), hot_res[1]], axis=0)
    y_rows = out_buf[buf_pos].reshape(EP * TOK, TOP, D).astype(jnp.float32)
    moe_out = jnp.sum(gate_vals[:, :, None] * y_rows, axis=1).astype(jnp.bfloat16)
    dx_rows = dx_buf[buf_pos].reshape(EP * TOK, TOP, D).astype(jnp.float32)
    grad_tokens = jnp.sum(dx_rows, axis=1).astype(jnp.bfloat16)
    grad_list = [cold_g.at[HOT].add(hot_g).astype(jnp.bfloat16) for cold_g, hot_g in zip(cold_res[2:], hot_res[2:])]
    return (moe_out, grad_tokens, grad_list[0], grad_list[1], grad_list[2])
```

```python
import functools
import math

import jax
import jax.numpy as jnp
from jax import lax
from jax.experimental import pallas as pl
from jax.experimental.pallas import tpu as pltpu
from jax.sharding import PartitionSpec as P

MESH = pl.DeviceIdType.MESH
F32 = jnp.float32
BF16 = jnp.bfloat16
NT = (((1,), (1,)), ((), ()))
NUM_COPIES = 120


def dot(lhs, rhs):
    return jnp.dot(lhs, rhs, preferred_element_type=F32)


def dot_nt(lhs, rhs):
    return lax.dot_general(lhs, rhs, NT, preferred_element_type=F32)


def gate_columns(gate_row, width):
    cols = jnp.transpose(jnp.broadcast_to(gate_row, (128, gate_row.shape[1])))
    return jnp.concatenate([cols] * (width // 128), axis=1)


def layer_kernel(side, x_ref, dy_ref, g_ref, w1_ref, w3_ref, w2_ref,
                 y_out, dx_out, dw1_out, dw3_out, dw2_out, xg, dg, gg, wg, rs_full,
                 wv, xrow, dyrow, grow, acc, rs_half, dw, xs, ds, gs, u_s, dab_s, do_s, xt_s,
                 send_sem, recv_sem, loc_sem):
    rows, width = x_ref.shape
    ff = w1_ref.shape[1]
    half = rows // 2
    fc = ff // 2
    nc = width // 4
    me = lax.axis_index("ep")
    core = lax.rem(me, 2)
    px = lax.rem(me // 2, side)
    py = me // (2 * side)

    def dev(yy, xx, cc):
        return (lax.rem(yy + side, side) * side + lax.rem(xx + side, side)) * 2 + cc

    xp, xm = dev(py, px + 1, core), dev(py, px - 1, core)
    yp, ym = dev(py + 1, px, core), dev(py - 1, px, core)
    partner = dev(py, px, 1 - core)

    copies = {}

    def reg(key, src, dst, target):
        k = len(copies)
        copies[key] = pltpu.make_async_remote_copy(
            src_ref=src, dst_ref=dst, send_sem=send_sem.at[k], recv_sem=recv_sem.at[k],
            device_id={"ep": target}, device_id_type=MESH)

    def reg_ring(key, plus, minus, src, buf, n):
        reg(key + ("+",), src, buf(2), plus)
        reg(key + ("-",), src, buf(1), minus)
        reg(key + ("2+",), buf(2).at[pl.ds(0, n // 2)], buf(3).at[pl.ds(0, n // 2)], plus)
        reg(key + ("2-",), buf(1).at[pl.ds(n // 2, n // 2)], buf(3).at[pl.ds(n // 2, n // 2)], minus)

    wn = wv.shape[1]
    reg_ring(("w",), yp, ym, wv.at[0], lambda s: wg.at[{1: 2, 2: 3, 3: 6}[s]], wn)
    reg(("wp", 0), wv.at[0], wg.at[1], partner)
    reg(("wp", 2), wg.at[2], wg.at[4], partner)
    reg(("wp", 3), wg.at[3], wg.at[5], partner)
    reg(("wp", 6), wg.at[6], wg.at[7], partner)
    for name, own, buf, n in (("x", x_ref, xg, rows), ("g", g_ref, gg, g_ref.shape[0])):
        reg_ring((name, 0), xp, xm, own, lambda s, buf=buf: buf.at[0, s, 0], n)
        for i in range(4):
            src = own if i == 0 else buf.at[0, i, 0]
            reg_ring((name, "y", i), yp, ym, src, lambda s, buf=buf, i=i: buf.at[s, i, 0], n)
    reg_ring(("d", "y"), yp, ym, dy_ref, lambda s: dg.at[s, 0, 0], rows)
    for j in range(4):
        src = dy_ref if j == 0 else dg.at[j, 0, 0]
        reg_ring(("d", j), xp, xm, src, lambda s, j=j: dg.at[j, s, 0], rows)
    for name, own, buf in (("x", x_ref, xg), ("g", g_ref, gg), ("d", dy_ref, dg)):
        for j in range(4):
            for i in range(4):
                reg((name + "p", j, i), own if (i, j) == (0, 0) else buf.at[j, i, 0], buf.at[j, i, 1], partner)
    reg(("r", "h+"), acc.at[3, :, pl.ds(0, half)], rs_half.at[0], xp)
    reg(("r", "h-"), acc.at[3, :, pl.ds(half, half)], rs_half.at[1], xm)
    reg(("r", "+"), acc.at[1], rs_full.at[0], xp)
    reg(("r", "-"), acc.at[2], rs_full.at[1], xm)

    def start(*keys):
        for key in keys:
            copies[key].start()

    def arrived(*keys):
        for key in keys:
            copies[key].wait_recv()

    def share(names, j, i):
        start(*[(name + "p", j, i) for name in names])

    def local(src, dst, k):
        return pltpu.make_async_copy(src, dst, loc_sem.at[k])

    w_loads = [local(w1_ref, wv.at[0, pl.ds(0, width), pl.ds(0, ff)], 0),
               local(w3_ref, wv.at[0, pl.ds(0, width), pl.ds(ff, ff)], 1),
               local(w2_ref, wv.at[0, pl.ds(width, ff)], 2)]
    t_loads = [local(x_ref, xrow.at[0], 3), local(dy_ref, dyrow.at[0], 4), local(g_ref, grow.at[0], 5)]
    for c in w_loads + t_loads:
        c.start()

    barrier = pltpu.get_barrier_semaphore()
    for target in (xp, xm, yp, ym, partner):
        pl.semaphore_signal(barrier, inc=1, device_id={"ep": target}, device_id_type=MESH)
    pl.semaphore_wait(barrier, 5)

    for name in ("g", "x", "d"):
        start((name, 0, "+"), (name, 0, "-"))
    for c in w_loads:
        c.wait()
    start(("w", "+"), ("w", "-"), ("wp", 0), ("d", "y", "+"), ("d", "y", "-"))
    share("gxd", 0, 0)
    for c in t_loads:
        c.wait()
    own_stores = [local(xrow.at[0], xg.at[0, 0, 0], 3), local(dyrow.at[0], dg.at[0, 0, 0], 4),
                  local(grow.at[0], gg.at[0, 0, 0], 5)]
    for c in own_stores:
        c.start()
    for b in range(4):
        for v in range(2):
            acc[b, v] = jnp.zeros((rows, width), F32)
    dw[...] = jnp.zeros_like(dw)

    def stage_row(i, k):
        return [local(xg.at[0, i, 0], xrow.at[i], k), local(dg.at[0, i, 0], dyrow.at[i], k + 1),
                local(gg.at[0, i, 0], grow.at[i], k + 2)]

    def stage_w(e, slot):
        return local(wg.at[e], wv.at[slot], 6 + slot)

    def acts(x, do, slot, h):
        a = dot(x, wv[slot, pl.ds(0, width), pl.ds(h * fc, fc)])
        b = dot(x, wv[slot, pl.ds(0, width), pl.ds(ff + h * fc, fc)])
        du = dot_nt(do, wv[slot, pl.ds(width + h * fc, fc), :])
        sig = jax.nn.sigmoid(a)
        hidden = a * sig * b
        da = du * b * sig * (1.0 + a * (1.0 - sig))
        db = du * a * sig
        return hidden, da, db

    def row_step(slot, i, jrel, plane):
        expert = dev(py + jrel, px, lax.rem(core + plane, 2))
        gate = gate_columns(grow[i, pl.ds(expert, 1), :], nc)
        routed = gate > 0.0
        for n in range(4):
            cols = pl.ds(n * nc, nc)
            do_s[pl.ds(0, rows), cols] = (gate * dyrow[i, :, cols].astype(F32)).astype(BF16)
        for h in range(2):
            hidden, da, db = acts(xrow[i], do_s[pl.ds(0, rows), :], slot, h)
            u_s[pl.ds(0, rows), pl.ds(h * fc, fc)] = hidden.astype(BF16)
            dab_s[pl.ds(0, rows), pl.ds(h * fc, fc)] = da.astype(BF16)
            dab_s[pl.ds(0, rows), pl.ds(ff + h * fc, fc)] = db.astype(BF16)
        for n in range(4):
            cols = pl.ds(n * nc, nc)
            o = dot(u_s[pl.ds(0, rows), :], wv[slot, pl.ds(width, ff), cols]).astype(BF16).astype(F32)
            acc[i, 0, :, cols] += jnp.where(routed, gate * o, 0.0)
            dxp = dot_nt(dab_s[pl.ds(0, rows), :], wv[slot, pl.ds(n * nc, nc), :]).astype(BF16).astype(F32)
            acc[i, 1, :, cols] += jnp.where(routed, dxp, 0.0)

    def first_steps(s, carry):
        i, e = s // 2, lax.rem(s, 2)

        @pl.when(s == 1)
        def _():
            arrived(("wp", 0))
            c = stage_w(1, 1)
            c.start()
            c.wait()

        @pl.when(s == 2)
        def _():
            for name in ("g", "x", "d"):
                arrived((name, 0, "+"), (name, 0, "-"))
                start((name, 0, "2+"), (name, 0, "2-"))
            share("gxd", 0, 1)
            share("gxd", 0, 2)
            cs = stage_row(1, 9) + stage_row(2, 12)
            for c in cs:
                c.start()
            for c in cs:
                c.wait()

        @pl.when(s == 6)
        def _():
            for name in ("g", "x", "d"):
                arrived((name, 0, "2+"), (name, 0, "2-"))
            share("gxd", 0, 3)
            cs = stage_row(3, 9)
            for c in cs:
                c.start()
            for c in cs:
                c.wait()

        row_step(e, i, 0, e)
        return carry

    lax.fori_loop(0, 8, first_steps, 0)

    arrived(("w", "+"), ("w", "-"))
    start(("w", "2+"), ("w", "2-"), ("wp", 2), ("wp", 3))
    stage_w(2, 2).start()

    def middle_steps(s, carry):
        k, i = s // 4, lax.rem(s, 4)
        slot = 2 - lax.rem(k, 2)

        @pl.when(i == 0)
        def _():
            stage_w(2, slot).wait()

        @pl.when(i == 3)
        def _():
            @pl.when(k == 0)
            def _():
                stage_w(3, 1).start()

            @pl.when(k == 1)
            def _():
                arrived(("wp", 2))
                stage_w(4, 2).start()

            @pl.when(k == 2)
            def _():
                arrived(("wp", 3))
                stage_w(5, 1).start()

            @pl.when(k == 3)
            def _():
                arrived(("w", "2+"), ("w", "2-"))
                start(("wp", 6))
                stage_w(6, 2).start()

        @pl.when(s == 2)
        def _():
            arrived(("d", "y", "+"), ("d", "y", "-"))
            start(("d", "y", "2+"), ("d", "y", "2-"))
            for j in (1, 2):
                start(("d", j, "+"), ("d", j, "-"))
                share("d", j, 0)
            for b in range(4):
                for name in ("g", "x"):
                    start((name, "y", b, "+"), (name, "y", b, "-"))

        @pl.when(s == 9)
        def _():
            arrived(("d", "y", "2+"), ("d", "y", "2-"))
            start(("d", 3, "+"), ("d", 3, "-"))
            share("d", 3, 0)

        for j, when in ((1, 11), (2, 14)):
            @pl.when(s == when)
            def _(j=j):
                arrived(("d", j, "+"), ("d", j, "-"))
                start(("d", j, "2+"), ("d", j, "2-"))
                share("d", j, 1)
                share("d", j, 2)

        row_step(slot, i, 1 + 2 * lax.rem(k, 2), k // 2)
        return carry

    lax.fori_loop(0, 16, middle_steps, 0)
    stage_w(6, 2).wait()

    def pass_on_x(b):
        for name in ("g", "x"):
            arrived((name, "y", b, "+"), (name, "y", b, "-"))
            start((name, "y", b, "2+"), (name, "y", b, "2-"))
        share("gx", 1, b)
        share("gx", 2, b)

    def last_steps(s, carry):
        i, e = 3 - s // 2, lax.rem(s, 2)

        @pl.when(s == 1)
        def _():
            arrived(("wp", 6))
            c = stage_w(7, 1)
            c.start()
            c.wait()

        @pl.when(s == 2)
        def _():
            start(("r", "h+"), ("r", "h-"))
            pass_on_x(0)

        @pl.when(s == 4)
        def _():
            arrived(("d", 3, "+"), ("d", 3, "-"))
            start(("d", 3, "2+"), ("d", 3, "2-"))
            share("d", 3, 1)
            share("d", 3, 2)
            pass_on_x(1)

        @pl.when(s == 6)
        def _():
            arrived(("r", "h+"), ("r", "h-"))
            acc[1, :, pl.ds(0, half), :] += rs_half[0]
            acc[2, :, pl.ds(half, half), :] += rs_half[1]
            start(("r", "+"), ("r", "-"))
            pass_on_x(2)

        row_step(2 - e, i, 2, e)
        return carry

    lax.fori_loop(0, 8, last_steps, 0)
    for c in own_stores:
        c.wait()

    def stage_pair(j, i, slot):
        return [local(xg.at[j, i], xs.at[slot], 9 + slot), local(dg.at[j, i], ds.at[slot], 11 + slot),
                local(gg.at[j, i], gs.at[slot], 13 + slot)]

    def get_pair(j, i):
        arrived(("xp", j, i), ("gp", j, i), ("dp", j, i))

    def grad_step(slot):
        gate = jnp.concatenate([gate_columns(gs[slot, p, pl.ds(me, 1), :], nc) for p in range(2)], axis=0)
        x = xs[slot].reshape(2 * rows, width)
        routed = gate[:, :fc] > 0.0 if nc >= fc else jnp.concatenate([gate] * (fc // nc), axis=1) > 0.0
        for n in range(4):
            cols = pl.ds(n * nc, nc)
            dy = ds[slot, :, :, cols].reshape(2 * rows, nc)
            do_s[:, cols] = (gate * dy.astype(F32)).astype(BF16)
        for h in range(2):
            hidden, da, db = acts(x, do_s[...], 0, h)
            u_s[:, pl.ds(h * fc, fc)] = jnp.where(routed, hidden, 0.0).astype(BF16)
            dab_s[:, pl.ds(h * fc, fc)] = jnp.where(routed, da, 0.0).astype(BF16)
            dab_s[:, pl.ds(ff + h * fc, fc)] = jnp.where(routed, db, 0.0).astype(BF16)
        xt_s[pl.ds(0, width), :] = jnp.transpose(x)
        xt_s[pl.ds(width, ff), :] = jnp.transpose(u_s[...])
        for n in range(4):
            cols = pl.ds(n * nc, nc)
            dw[pl.ds(0, width), cols] += dot(xt_s[pl.ds(0, width), :], dab_s[:, cols])
            dw[pl.ds(width, ff), cols] += dot(xt_s[pl.ds(width, ff), :], do_s[:, cols])

    get_pair(0, 0)
    for c in stage_pair(0, 0, 0):
        c.start()

    def grad_steps(q, carry):
        slot = lax.rem(q, 2)
        nxt = q + 1
        nj, ni = nxt // 4, lax.rem(nxt, 4)

        @pl.when(q == 0)
        def _():
            pass_on_x(3)

        for step in range(1, 16):
            j, i = step // 4, step % 4

            @pl.when(q == step - 1)
            def _(j=j, i=i):
                if j == 1 and i == 0:
                    for jj in (1, 2, 3):
                        arrived(("d", jj, "2+"), ("d", jj, "2-"))
                        share("d", jj, 3)
                if j == 2:
                    for name in ("g", "x"):
                        arrived((name, "y", i, "2+"), (name, "y", i, "2-"))
                    share("gx", 3, i)
                get_pair(j, i)

        @pl.when(q < 15)
        def _():
            for c in stage_pair(nj, ni, 1 - slot):
                c.start()

        for c in stage_pair(0, 0, slot):
            c.wait()
        grad_step(slot)
        return carry

    lax.fori_loop(0, 16, grad_steps, 0)

    outs = []
    wv[1] = dw[...].astype(BF16)
    outs += [local(wv.at[1, pl.ds(0, width), pl.ds(0, ff)], dw1_out, 0),
             local(wv.at[1, pl.ds(0, width), pl.ds(ff, ff)], dw3_out, 1),
             local(wv.at[1, pl.ds(width, ff)], dw2_out, 2)]
    for c in outs:
        c.start()
    arrived(("r", "+"), ("r", "-"))
    copies[("r", "+")].wait_send()
    copies[("r", "-")].wait_send()
    fetch = [local(rs_full.at[0], acc.at[1], 3), local(rs_full.at[1], acc.at[2], 4)]
    for c in fetch:
        c.start()
    for c in fetch:
        c.wait()
    for v, (buf, out) in enumerate(((xrow, y_out), (dyrow, dx_out))):
        buf[1] = (acc[0, v] + acc[1, v] + acc[2, v]).astype(BF16)
        c = local(buf.at[1], out, 3 + v)
        c.start()
        outs.append(c)
    for key, c in copies.items():
        if key not in (("r", "+"), ("r", "-")):
            c.wait_send()
    for c in outs:
        c.wait()


def solution(mesh):
    group_size = mesh.shape["ep"]
    side = math.isqrt(group_size // 2)
    tok_spec = P(("dp", "ep"), None)
    w_spec = P("ep", None, None)
    grad_spec = P(("dp", "ep"), None, None)

    def device_fn(x, ids, gates, w1, w3, w2, dy):
        rows, width = x.shape
        ff = w1.shape[2]
        experts = group_size * w1.shape[0]
        onehot = ids[None, :, :] == jnp.arange(experts, dtype=ids.dtype)[:, None, None]
        gate_t = jnp.sum(jnp.where(onehot, gates[None, :, :], 0.0), axis=2)
        any_spec = pl.BlockSpec(memory_space=pl.ANY)
        sds = jax.ShapeDtypeStruct
        out_shape = (
            sds((rows, width), BF16), sds((rows, width), BF16),
            sds((width, ff), BF16), sds((width, ff), BF16), sds((ff, width), BF16),
            sds((4, 4, 2, rows, width), BF16), sds((4, 4, 2, rows, width), BF16),
            sds((4, 4, 2, experts, rows), F32), sds((8, width + ff, width), BF16),
            sds((2, 2, rows, width), F32))
        vmem = pltpu.VMEM
        outs = pl.pallas_call(
            functools.partial(layer_kernel, side),
            out_shape=out_shape,
            in_specs=[any_spec] * 6,
            out_specs=[any_spec] * len(out_shape),
            scratch_shapes=[
                vmem((3, width + ff, width), BF16),
                vmem((4, rows, width), BF16), vmem((4, rows, width), BF16), vmem((4, experts, rows), F32),
                vmem((4, 2, rows, width), F32), vmem((2, 2, rows // 2, width), F32),
                vmem((width + ff, width), F32),
                vmem((2, 2, rows, width), BF16), vmem((2, 2, rows, width), BF16), vmem((2, 2, experts, rows), F32),
                vmem((2 * rows, ff), BF16), vmem((2 * rows, 2 * ff), BF16), vmem((2 * rows, width), BF16),
                vmem((width + ff, 2 * rows), BF16),
                pltpu.SemaphoreType.DMA((NUM_COPIES,)), pltpu.SemaphoreType.DMA((NUM_COPIES,)),
                pltpu.SemaphoreType.DMA((15,)),
            ],
            compiler_params=pltpu.CompilerParams(
                collective_id=0, has_side_effects=True, vmem_limit_bytes=66_900_000),
        )(x, dy, gate_t, w1[0], w3[0], w2[0])
        return outs[0], outs[1], outs[2][None], outs[3][None], outs[4][None]

    def layer_fn(tokens, expert_ids, gate_vals, w_gate, w_up, w_down, grad_out):
        return jax.shard_map(
            device_fn, mesh=mesh,
            in_specs=(tok_spec, tok_spec, tok_spec, w_spec, w_spec, w_spec, tok_spec),
            out_specs=(tok_spec, tok_spec, grad_spec, grad_spec, grad_spec), check_vma=False,
        )(tokens, expert_ids, gate_vals, w_gate, w_up, w_down, grad_out)

    return layer_fn
```

```python
import functools
import math

import jax
import jax.numpy as jnp
from jax import lax
from jax.experimental import pallas as pl
from jax.experimental.pallas import tpu as pltpu
from jax.sharding import PartitionSpec as P

MESH = pl.DeviceIdType.MESH
F32 = jnp.float32
BF16 = jnp.bfloat16
NT = (((1,), (1,)), ((), ()))
NUM_COPIES = 122


def dot(lhs, rhs):
    return jnp.dot(lhs, rhs, preferred_element_type=F32)


def dot_nt(lhs, rhs):
    return lax.dot_general(lhs, rhs, NT, preferred_element_type=F32)


def gate_columns(gate_row, width):
    cols = jnp.transpose(jnp.broadcast_to(gate_row, (128, gate_row.shape[1])))
    return jnp.concatenate([cols] * (width // 128), axis=1)


def layer_kernel(side, x_ref, dy_ref, g_ref, w1_ref, w3_ref, w2_ref,
                 y_out, dx_out, dw1_out, dw3_out, dw2_out, xg, dg, gg, wg, rs_full,
                 wv, xrow, dyrow, grow, acc, rs_half, dw, xs, ds, gs, u_s, dab_s, do_s, xt_s,
                 send_sem, recv_sem, loc_sem):
    rows, width = x_ref.shape
    ff = w1_ref.shape[1]
    half = rows // 2
    fc = ff // 2
    nc = width // 4
    me = lax.axis_index("ep")
    core = lax.rem(me, 2)
    px = lax.rem(me // 2, side)
    py = me // (2 * side)

    def dev(yy, xx, cc):
        return (lax.rem(yy + side, side) * side + lax.rem(xx + side, side)) * 2 + cc

    xp, xm = dev(py, px + 1, core), dev(py, px - 1, core)
    yp, ym = dev(py + 1, px, core), dev(py - 1, px, core)
    partner = dev(py, px, 1 - core)

    copies = {}

    def reg(key, src, dst, target):
        k = len(copies)
        copies[key] = pltpu.make_async_remote_copy(
            src_ref=src, dst_ref=dst, send_sem=send_sem.at[k], recv_sem=recv_sem.at[k],
            device_id={"ep": target}, device_id_type=MESH)

    def reg_ring(key, plus, minus, src, buf, n):
        reg(key + ("+",), src, buf(2), plus)
        reg(key + ("-",), src, buf(1), minus)
        reg(key + ("2+",), buf(2).at[pl.ds(0, n // 2)], buf(3).at[pl.ds(0, n // 2)], plus)
        reg(key + ("2-",), buf(1).at[pl.ds(n // 2, n // 2)], buf(3).at[pl.ds(n // 2, n // 2)], minus)

    wn = wv.shape[1]
    reg_ring(("w",), yp, ym, wv.at[0], lambda s: wg.at[{1: 2, 2: 3, 3: 6}[s]], wn)
    reg(("wp", 0), wv.at[0], wg.at[1], partner)
    reg(("wp", 2), wg.at[2], wg.at[4], partner)
    reg(("wp", 3), wg.at[3], wg.at[5], partner)
    reg(("wp", 6), wg.at[6], wg.at[7], partner)
    for name, own, buf, n in (("x", x_ref, xg, rows), ("g", g_ref, gg, g_ref.shape[0])):
        reg_ring((name, 0), xp, xm, own, lambda s, buf=buf: buf.at[0, s, 0], n)
        for i in range(4):
            src = own if i == 0 else buf.at[0, i, 0]
            reg_ring((name, "y", i), yp, ym, src, lambda s, buf=buf, i=i: buf.at[s, i, 0], n)
    reg_ring(("d", "y"), yp, ym, dy_ref, lambda s: dg.at[s, 0, 0], rows)
    for j in range(4):
        src = dy_ref if j == 0 else dg.at[j, 0, 0]
        reg_ring(("d", j), xp, xm, src, lambda s, j=j: dg.at[j, s, 0], rows)
    for name, own, buf in (("x", x_ref, xg), ("g", g_ref, gg), ("d", dy_ref, dg)):
        for j in range(4):
            for i in range(4):
                reg((name + "p", j, i), own if (i, j) == (0, 0) else buf.at[j, i, 0], buf.at[j, i, 1], partner)
    reg(("r", "h+"), acc.at[3, :, pl.ds(0, half)], rs_half.at[0], xp)
    reg(("r", "h-"), acc.at[3, :, pl.ds(half, half)], rs_half.at[1], xm)
    lo, hi = pl.ds(0, half), pl.ds(half, half)
    reg(("r", "+a"), acc.at[1, :, hi], rs_full.at[0, :, hi], xp)
    reg(("r", "-a"), acc.at[2, :, lo], rs_full.at[1, :, lo], xm)
    reg(("r", "+b"), acc.at[1, :, lo], rs_full.at[0, :, lo], xp)
    reg(("r", "-b"), acc.at[2, :, hi], rs_full.at[1, :, hi], xm)

    def start(*keys):
        for key in keys:
            copies[key].start()

    def arrived(*keys):
        for key in keys:
            copies[key].wait_recv()

    def share(names, j, i):
        start(*[(name + "p", j, i) for name in names])

    def local(src, dst, k):
        return pltpu.make_async_copy(src, dst, loc_sem.at[k])

    w_loads = [local(w1_ref, wv.at[0, pl.ds(0, width), pl.ds(0, ff)], 0),
               local(w3_ref, wv.at[0, pl.ds(0, width), pl.ds(ff, ff)], 1),
               local(w2_ref, wv.at[0, pl.ds(width, ff)], 2)]
    t_loads = [local(x_ref, xrow.at[0], 3), local(dy_ref, dyrow.at[0], 4), local(g_ref, grow.at[0], 5)]
    for c in w_loads + t_loads:
        c.start()

    barrier = pltpu.get_barrier_semaphore()
    for target in (xp, xm, yp, ym, partner):
        pl.semaphore_signal(barrier, inc=1, device_id={"ep": target}, device_id_type=MESH)
    pl.semaphore_wait(barrier, 5)

    start(("d", "y", "+"), ("d", "y", "-"))
    for name in ("g", "x", "d"):
        start((name, 0, "+"), (name, 0, "-"))
    for c in w_loads:
        c.wait()
    start(("w", "+"), ("w", "-"), ("wp", 0))
    share("gxd", 0, 0)
    for c in t_loads:
        c.wait()
    own_stores = [local(xrow.at[0], xg.at[0, 0, 0], 3), local(dyrow.at[0], dg.at[0, 0, 0], 4),
                  local(grow.at[0], gg.at[0, 0, 0], 5)]
    for c in own_stores:
        c.start()
    for b in range(4):
        for v in range(2):
            acc[b, v] = jnp.zeros((rows, width), F32)
    dw[...] = jnp.zeros_like(dw)

    def stage_row(i, k):
        return [local(xg.at[0, i, 0], xrow.at[i], k), local(dg.at[0, i, 0], dyrow.at[i], k + 1),
                local(gg.at[0, i, 0], grow.at[i], k + 2)]

    def stage_w(e, slot):
        return local(wg.at[e], wv.at[slot], 6 + slot)

    def acts(x, do, slot, h):
        a = dot(x, wv[slot, pl.ds(0, width), pl.ds(h * fc, fc)])
        b = dot(x, wv[slot, pl.ds(0, width), pl.ds(ff + h * fc, fc)])
        du = dot_nt(do, wv[slot, pl.ds(width + h * fc, fc), :])
        sig = jax.nn.sigmoid(a)
        hidden = a * sig * b
        da = du * b * sig * (1.0 + a * (1.0 - sig))
        db = du * a * sig
        return hidden, da, db

    def row_step(slot, i, jrel, plane):
        expert = dev(py + jrel, px, lax.rem(core + plane, 2))
        gate = gate_columns(grow[i, pl.ds(expert, 1), :], nc)
        routed = gate > 0.0
        for n in range(4):
            cols = pl.ds(n * nc, nc)
            do_s[pl.ds(0, rows), cols] = (gate * dyrow[i, :, cols].astype(F32)).astype(BF16)
        for h in range(2):
            hidden, da, db = acts(xrow[i], do_s[pl.ds(0, rows), :], slot, h)
            u_s[pl.ds(0, rows), pl.ds(h * fc, fc)] = hidden.astype(BF16)
            dab_s[pl.ds(0, rows), pl.ds(h * fc, fc)] = da.astype(BF16)
            dab_s[pl.ds(0, rows), pl.ds(ff + h * fc, fc)] = db.astype(BF16)
        for n in range(4):
            cols = pl.ds(n * nc, nc)
            o = dot(u_s[pl.ds(0, rows), :], wv[slot, pl.ds(width, ff), cols]).astype(BF16).astype(F32)
            acc[i, 0, :, cols] += jnp.where(routed, gate * o, 0.0)
            dxp = dot_nt(dab_s[pl.ds(0, rows), :], wv[slot, pl.ds(n * nc, nc), :]).astype(BF16).astype(F32)
            acc[i, 1, :, cols] += jnp.where(routed, dxp, 0.0)

    def run(copies_):
        for c in copies_:
            c.start()
        for c in copies_:
            c.wait()

    def at_steps(s, pumps):
        for k, pump in pumps.items():
            pl.when(s == k)(pump)

    def forward(name, key):
        arrived((name, key, "+"), (name, key, "-"))
        start((name, key, "2+"), (name, key, "2-"))

    def partner_weights():
        arrived(("wp", 0))
        run([stage_w(1, 1)])

    def row_neighbours():
        for name in ("g", "x", "d"):
            forward(name, 0)
        arrived(("d", "y", "+"), ("d", "y", "-"))
        start(("d", "y", "2+"), ("d", "y", "2-"))
        for j in (1, 2):
            start(("d", j, "+"), ("d", j, "-"))
        for i in (1, 2):
            share("gxd", 0, i)
        run(stage_row(1, 9) + stage_row(2, 12))
        for j in (1, 2):
            share("d", j, 0)

    def row_far():
        for name in ("g", "x", "d"):
            arrived((name, 0, "2+"), (name, 0, "2-"))
        share("gxd", 0, 3)
        run(stage_row(3, 9))

    def first_steps(s, carry):
        i, e = s // 2, lax.rem(s, 2)
        at_steps(s, {1: partner_weights, 2: row_neighbours, 6: row_far})
        row_step(e, i, 0, e)
        return carry

    lax.fori_loop(0, 8, first_steps, 0)
    for c in own_stores:
        c.wait()

    def stage_pair(j, i, slot):
        return [local(xg.at[j, i], xs.at[slot], 9 + slot), local(dg.at[j, i], ds.at[slot], 11 + slot),
                local(gg.at[j, i], gs.at[slot], 13 + slot)]

    def get_pair(j, i, slot):
        arrived(("xp", j, i), ("gp", j, i), ("dp", j, i))
        for c in stage_pair(j, i, slot):
            c.start()

    def grad_step(slot):
        for c in stage_pair(0, 0, slot):
            c.wait()
        gate = jnp.concatenate([gate_columns(gs[slot, p, pl.ds(me, 1), :], nc) for p in range(2)], axis=0)
        x = xs[slot].reshape(2 * rows, width)
        routed = gate[:, :fc] > 0.0 if nc >= fc else jnp.concatenate([gate] * (fc // nc), axis=1) > 0.0
        for n in range(4):
            cols = pl.ds(n * nc, nc)
            dy = ds[slot, :, :, cols].reshape(2 * rows, nc)
            do_s[:, cols] = (gate * dy.astype(F32)).astype(BF16)
        for h in range(2):
            hidden, da, db = acts(x, do_s[...], 0, h)
            u_s[:, pl.ds(h * fc, fc)] = jnp.where(routed, hidden, 0.0).astype(BF16)
            dab_s[:, pl.ds(h * fc, fc)] = jnp.where(routed, da, 0.0).astype(BF16)
            dab_s[:, pl.ds(ff + h * fc, fc)] = jnp.where(routed, db, 0.0).astype(BF16)
        xt_s[pl.ds(0, width), :] = jnp.transpose(x)
        xt_s[pl.ds(width, ff), :] = jnp.transpose(u_s[...])
        for n in range(4):
            cols = pl.ds(n * nc, nc)
            dw[pl.ds(0, width), cols] += dot(xt_s[pl.ds(0, width), :], dab_s[:, cols])
            dw[pl.ds(width, ff), cols] += dot(xt_s[pl.ds(width, ff), :], do_s[:, cols])

    get_pair(0, 0, 0)

    def own_row_grads(q, carry):
        at_steps(q, {i - 1: functools.partial(get_pair, 0, i, i % 2) for i in range(1, 4)})
        grad_step(lax.rem(q, 2))
        return carry

    lax.fori_loop(0, 4, own_row_grads, 0)

    forward("d", 1)
    for i in (1, 2):
        share("d", 1, i)
    arrived(("w", "+"), ("w", "-"))
    start(("w", "2+"), ("w", "2-"), ("wp", 2), ("wp", 3))
    stage_w(2, 2).start()
    for b in range(4):
        for name in ("g", "x"):
            start((name, "y", b, "+"), (name, "y", b, "-"))
    forward("d", 2)
    for i in (1, 2):
        share("d", 2, i)

    def cotangents_far():
        arrived(("d", "y", "2+"), ("d", "y", "2-"))
        start(("d", 3, "+"), ("d", 3, "-"))
        share("d", 3, 0)

    def cotangents_last():
        forward("d", 3)
        for i in (1, 2):
            share("d", 3, i)

    def next_weights(e):
        if e == 6:
            arrived(("w", "2+"), ("w", "2-"))
            start(("wp", 6))
        elif e > 3:
            arrived(("wp", e - 2))
        stage_w(e, 2 - e % 2).start()

    def middle_steps(s, carry):
        k, i = s // 4, lax.rem(s, 4)
        slot = 2 - lax.rem(k, 2)

        @pl.when(i == 0)
        def _():
            stage_w(2, slot).wait()

        at_steps(s, {3: functools.partial(next_weights, 3), 4: cotangents_far, 7: functools.partial(next_weights, 4),
                     11: functools.partial(next_weights, 5), 14: cotangents_last, 15: functools.partial(next_weights, 6)})
        row_step(slot, i, 1 + 2 * lax.rem(k, 2), k // 2)
        return carry

    lax.fori_loop(0, 16, middle_steps, 0)
    stage_w(6, 2).wait()

    def far_weights():
        arrived(("wp", 6))
        run([stage_w(7, 1)])

    def far_sums():
        start(("r", "h+"), ("r", "h-"))
        for j in (1, 2, 3):
            arrived(("d", j, "2+"), ("d", j, "2-"))
            share("d", j, 3)

    def pass_on_x(b):
        for name in ("g", "x"):
            forward_y(name, b)
        share("gx", 1, b)
        share("gx", 2, b)

    def forward_y(name, b):
        arrived((name, "y", b, "+"), (name, "y", b, "-"))
        start((name, "y", b, "2+"), (name, "y", b, "2-"))

    def last_steps(s, carry):
        i, e = 3 - s // 2, lax.rem(s, 2)
        at_steps(s, {1: far_weights, 2: far_sums, 4: lambda: start(("r", "-a")), 6: lambda: start(("r", "+a"))})
        row_step(2 - e, i, 2, e)
        return carry

    lax.fori_loop(0, 8, last_steps, 0)

    def far_x(b):
        for name in ("g", "x"):
            arrived((name, "y", b, "2+"), (name, "y", b, "2-"))
        share("gx", 3, b)

    def pass_on_sums():
        arrived(("r", "h+"), ("r", "h-"))
        acc[1, :, lo, :] += rs_half[0]
        acc[2, :, hi, :] += rs_half[1]
        start(("r", "+b"), ("r", "-b"))

    pairs = [(1 + q % 2, q // 2) for q in range(8)] + [(3, b) for b in range(4)]
    pass_on_x(0)
    get_pair(1, 0, 0)

    def before_grad(q):
        nj, ni = pairs[q + 1]
        if nj == 2:
            get_pair(nj, ni, (q + 1) % 2)

    def after_grad(q):
        nj, ni = pairs[q + 1]
        if nj == 1:
            pass_on_x(ni)
        if nj == 3:
            far_x(ni)
        if nj != 2:
            get_pair(nj, ni, (q + 1) % 2)

    def grad_steps(q, carry):
        at_steps(q, {4: pass_on_sums})
        at_steps(q, {k: functools.partial(before_grad, k) for k in range(11)})
        grad_step(lax.rem(q, 2))
        at_steps(q, {k: functools.partial(after_grad, k) for k in range(11)})
        return carry

    lax.fori_loop(0, 12, grad_steps, 0)

    outs = []
    wv[1] = dw[...].astype(BF16)
    outs += [local(wv.at[1, pl.ds(0, width), pl.ds(0, ff)], dw1_out, 0),
             local(wv.at[1, pl.ds(0, width), pl.ds(ff, ff)], dw3_out, 1),
             local(wv.at[1, pl.ds(width, ff)], dw2_out, 2)]
    for c in outs:
        c.start()
    sums = [("r", "+a"), ("r", "-a"), ("r", "+b"), ("r", "-b")]
    arrived(*sums)
    for key in sums:
        copies[key].wait_send()
    fetch = [local(rs_full.at[0], acc.at[1], 3), local(rs_full.at[1], acc.at[2], 4)]
    for c in fetch:
        c.start()
    for c in fetch:
        c.wait()
    for v, (buf, out) in enumerate(((xrow, y_out), (dyrow, dx_out))):
        buf[1] = (acc[0, v] + acc[1, v] + acc[2, v]).astype(BF16)
        c = local(buf.at[1], out, 3 + v)
        c.start()
        outs.append(c)
    for key, c in copies.items():
        if key not in sums:
            c.wait_send()
    for c in outs:
        c.wait()


def copy_kernel(*refs):
    n = (len(refs) - 1) // 3
    srcs, dsts, bufs = refs[:n], refs[n:2 * n], refs[2 * n:3 * n]
    sem = refs[3 * n]
    ins = [pltpu.make_async_copy(s, b, sem.at[0, k]) for k, (s, b) in enumerate(zip(srcs, bufs))]
    outs = [pltpu.make_async_copy(b, d, sem.at[1, k]) for k, (b, d) in enumerate(zip(bufs, dsts))]
    for c in ins:
        c.start()
    for i, o in zip(ins, outs):
        i.wait()
        o.start()
    for o in outs:
        o.wait()


def solution(mesh):
    group_size = mesh.shape["ep"]
    side = math.isqrt(group_size // 2)
    tok_spec = P(("dp", "ep"), None)
    w_spec = P("ep", None, None)
    grad_spec = P(("dp", "ep"), None, None)

    def device_fn(x, ids, gates, w1, w3, w2, dy):
        rows, width = x.shape
        ff = w1.shape[2]
        experts = group_size * w1.shape[0]
        onehot = ids[None, :, :] == jnp.arange(experts, dtype=ids.dtype)[:, None, None]
        gate_t = jnp.sum(jnp.where(onehot, gates[None, :, :], 0.0), axis=2)
        any_spec = pl.BlockSpec(memory_space=pl.ANY)
        sds = jax.ShapeDtypeStruct
        out_shape = (
            sds((rows, width), BF16), sds((rows, width), BF16),
            sds((width, ff), BF16), sds((width, ff), BF16), sds((ff, width), BF16),
            sds((4, 4, 2, rows, width), BF16), sds((4, 4, 2, rows, width), BF16),
            sds((4, 4, 2, experts, rows), F32), sds((8, width + ff, width), BF16),
            sds((2, 2, rows, width), F32))
        vmem = pltpu.VMEM
        outs = pl.pallas_call(
            functools.partial(layer_kernel, side),
            out_shape=out_shape,
            in_specs=[any_spec] * 6,
            out_specs=[any_spec] * len(out_shape),
            scratch_shapes=[
                vmem((3, width + ff, width), BF16),
                vmem((4, rows, width), BF16), vmem((4, rows, width), BF16), vmem((4, experts, rows), F32),
                vmem((4, 2, rows, width), F32), vmem((2, 2, rows // 2, width), F32),
                vmem((width + ff, width), F32),
                vmem((2, 2, rows, width), BF16), vmem((2, 2, rows, width), BF16), vmem((2, 2, experts, rows), F32),
                vmem((2 * rows, ff), BF16), vmem((2 * rows, 2 * ff), BF16), vmem((2 * rows, width), BF16),
                vmem((width + ff, 2 * rows), BF16),
                pltpu.SemaphoreType.DMA((NUM_COPIES,)), pltpu.SemaphoreType.DMA((NUM_COPIES,)),
                pltpu.SemaphoreType.DMA((15,)),
            ],
            compiler_params=pltpu.CompilerParams(
                collective_id=0, has_side_effects=True, vmem_limit_bytes=66_900_000),
        )(x, dy, gate_t, w1[0], w3[0], w2[0])
        outs = outs[:5]
        y, dx, dw1, dw3, dw2 = pl.pallas_call(
            copy_kernel,
            out_shape=[sds(o.shape, o.dtype) for o in outs],
            in_specs=[any_spec] * 5,
            out_specs=[any_spec] * 5,
            scratch_shapes=[vmem(o.shape, o.dtype) for o in outs] + [pltpu.SemaphoreType.DMA((2, 5))],
        )(*outs)
        return y, dx, dw1[None], dw3[None], dw2[None]

    def layer_fn(tokens, expert_ids, gate_vals, w_gate, w_up, w_down, grad_out):
        return jax.shard_map(
            device_fn, mesh=mesh,
            in_specs=(tok_spec, tok_spec, tok_spec, w_spec, w_spec, w_spec, tok_spec),
            out_specs=(tok_spec, tok_spec, grad_spec, grad_spec, grad_spec), check_vma=False,
        )(tokens, expert_ids, gate_vals, w_gate, w_up, w_down, grad_out)

    return layer_fn
```

```python
import functools
import math

import jax
import jax.numpy as jnp
from jax import lax
from jax.experimental import pallas as pl
from jax.experimental.pallas import tpu as pltpu
from jax.sharding import PartitionSpec as P

MESH = pl.DeviceIdType.MESH
F32 = jnp.float32
BF16 = jnp.bfloat16
NT = (((1,), (1,)), ((), ()))
NUM_COPIES = 101


def dot(lhs, rhs):
    return jnp.dot(lhs, rhs, preferred_element_type=F32)


def dot_nt(lhs, rhs):
    return lax.dot_general(lhs, rhs, NT, preferred_element_type=F32)


def gate_columns(gate_row, width):
    cols = jnp.transpose(jnp.broadcast_to(gate_row, (128, gate_row.shape[1])))
    return jnp.concatenate([cols] * (width // 128), axis=1)


def layer_kernel(side, x_ref, dy_ref, g_ref, w1_ref, w3_ref, w2_ref,
                 y_out, dx_out, dw1_out, dw3_out, dw2_out, xg, dg, gg, gy, wg,
                 wv, xrow, dyrow, grow, acc, rs_half, rs_full, dw, xs, ds, gs, u_s, dab_s, do_s, xt_s,
                 send_sem, recv_sem, loc_sem):
    rows, width = x_ref.shape
    ff = w1_ref.shape[1]
    half = rows // 2
    fc = ff // 2
    nc = width // 4
    me = lax.axis_index("ep")
    core = lax.rem(me, 2)
    px = lax.rem(me // 2, side)
    py = me // (2 * side)

    def dev(yy, xx, cc):
        return (lax.rem(yy + side, side) * side + lax.rem(xx + side, side)) * 2 + cc

    xp, xm = dev(py, px + 1, core), dev(py, px - 1, core)
    yp, ym = dev(py + 1, px, core), dev(py - 1, px, core)
    partner = dev(py, px, 1 - core)

    copies = {}

    def reg(key, src, dst, target):
        k = len(copies)
        copies[key] = pltpu.make_async_remote_copy(
            src_ref=src, dst_ref=dst, send_sem=send_sem.at[k], recv_sem=recv_sem.at[k],
            device_id={"ep": target}, device_id_type=MESH)

    def reg_ring(key, plus, minus, src, buf, n):
        reg(key + ("+",), src, buf(2), plus)
        reg(key + ("-",), src, buf(1), minus)
        reg(key + ("2+",), buf(2).at[pl.ds(0, n // 2)], buf(3).at[pl.ds(0, n // 2)], plus)
        reg(key + ("2-",), buf(1).at[pl.ds(n // 2, n // 2)], buf(3).at[pl.ds(n // 2, n // 2)], minus)

    wn = wv.shape[1]
    reg_ring(("w",), yp, ym, wv.at[0], lambda s: wg.at[{1: 2, 2: 3, 3: 6}[s]], wn)
    reg(("wp", 0), wv.at[0], wg.at[1], partner)
    reg(("wp", 2), wg.at[2], wg.at[4], partner)
    reg(("wp", 3), wg.at[3], wg.at[5], partner)
    reg(("wp", 6), wg.at[6], wg.at[7], partner)
    column = pl.ds(pl.multiple_of(px * (2 * side), 2 * side), 2 * side)
    reg_ring(("x", 0), xp, xm, x_ref, lambda s: xg.at[0, s, 0], rows)
    reg_ring(("g", 0), xp, xm, g_ref, lambda s: gg.at[s, 0], g_ref.shape[0])
    for i in range(4):
        src = x_ref if i == 0 else xg.at[0, i, 0]
        reg_ring(("x", "y", i), yp, ym, src, lambda s, i=i: xg.at[s, i, 0], rows)
    reg_ring(("g", "y"), yp, ym, gg.at[:, 0, column], lambda s: gy.at[s, 0], 4)
    reg_ring(("d", "y"), yp, ym, dy_ref, lambda s: dg.at[s, 0, 0], rows)
    for j in range(4):
        src = dy_ref if j == 0 else dg.at[j, 0, 0]
        reg_ring(("d", j), xp, xm, src, lambda s, j=j: dg.at[j, s, 0], rows)
    for j in range(4):
        for i in range(4):
            reg(("xp", j, i), x_ref if (i, j) == (0, 0) else xg.at[j, i, 0], xg.at[j, i, 1], partner)
            reg(("dp", j, i), dy_ref if (i, j) == (0, 0) else dg.at[j, i, 0], dg.at[j, i, 1], partner)
        reg(("gp", 0, j), g_ref if j == 0 else gg.at[j, 0], gg.at[j, 1], partner)
        if j:
            reg(("gyp", j), gy.at[j, 0], gy.at[j, 1], partner)
    reg(("r", "h+"), acc.at[3, :, pl.ds(0, half)], rs_half.at[0], xp)
    reg(("r", "h-"), acc.at[3, :, pl.ds(half, half)], rs_half.at[1], xm)
    lo, hi = pl.ds(0, half), pl.ds(half, half)
    reg(("r", "+a"), acc.at[1, :, hi], rs_full.at[0, :, hi], xp)
    reg(("r", "-a"), acc.at[2, :, lo], rs_full.at[1, :, lo], xm)
    reg(("r", "+b"), acc.at[1, :, lo], rs_full.at[0, :, lo], xp)
    reg(("r", "-b"), acc.at[2, :, hi], rs_full.at[1, :, hi], xm)

    def start(*keys):
        for key in keys:
            copies[key].start()

    def arrived(*keys):
        for key in keys:
            copies[key].wait_recv()

    def share(names, j, i):
        start(*[(name + "p", j, i) for name in names])

    def local(src, dst, k):
        return pltpu.make_async_copy(src, dst, loc_sem.at[k])

    w_loads = [local(w1_ref, wv.at[0, pl.ds(0, width), pl.ds(0, ff)], 0),
               local(w3_ref, wv.at[0, pl.ds(0, width), pl.ds(ff, ff)], 1),
               local(w2_ref, wv.at[0, pl.ds(width, ff)], 2)]
    t_loads = [local(x_ref, xrow.at[0], 3), local(dy_ref, dyrow.at[0], 4), local(g_ref, grow.at[0], 5)]
    for c in w_loads + t_loads:
        c.start()

    barrier = pltpu.get_barrier_semaphore()
    for target in (xp, xm, yp, ym, partner):
        pl.semaphore_signal(barrier, inc=1, device_id={"ep": target}, device_id_type=MESH)
    pl.semaphore_wait(barrier, 5)

    start(("d", "y", "+"), ("d", "y", "-"))
    for name in ("g", "x", "d"):
        start((name, 0, "+"), (name, 0, "-"))
    for c in w_loads:
        c.wait()
    start(("w", "+"), ("w", "-"), ("wp", 0))
    share("gxd", 0, 0)
    for c in t_loads:
        c.wait()
    own_stores = [local(xrow.at[0], xg.at[0, 0, 0], 3), local(dyrow.at[0], dg.at[0, 0, 0], 4),
                  local(grow.at[0], gg.at[0, 0], 5)]
    for c in own_stores:
        c.start()
    for b in range(4):
        for v in range(2):
            acc[b, v] = jnp.zeros((rows, width), F32)
    dw[...] = jnp.zeros_like(dw)

    def stage_row(i, k):
        return [local(xg.at[0, i, 0], xrow.at[i], k), local(dg.at[0, i, 0], dyrow.at[i], k + 1),
                local(gg.at[i, 0], grow.at[i], k + 2)]

    def stage_w(e, slot):
        return local(wg.at[e], wv.at[slot], 6 + slot)

    def acts(x, do, slot, h):
        a = dot(x, wv[slot, pl.ds(0, width), pl.ds(h * fc, fc)])
        b = dot(x, wv[slot, pl.ds(0, width), pl.ds(ff + h * fc, fc)])
        du = dot_nt(do, wv[slot, pl.ds(width + h * fc, fc), :])
        sig = jax.nn.sigmoid(a)
        hidden = a * sig * b
        da = du * b * sig * (1.0 + a * (1.0 - sig))
        db = du * a * sig
        return hidden, da, db

    def row_step(slot, i, jrel, plane):
        expert = (px * side + lax.rem(py + jrel, side)) * 2 + lax.rem(core + plane, 2)
        gate = gate_columns(grow[i, pl.ds(expert, 1), :], nc)
        routed = gate > 0.0
        for n in range(4):
            cols = pl.ds(n * nc, nc)
            do_s[pl.ds(0, rows), cols] = (gate * dyrow[i, :, cols].astype(F32)).astype(BF16)
        for h in range(2):
            hidden, da, db = acts(xrow[i], do_s[pl.ds(0, rows), :], slot, h)
            u_s[pl.ds(0, rows), pl.ds(h * fc, fc)] = hidden.astype(BF16)
            dab_s[pl.ds(0, rows), pl.ds(h * fc, fc)] = da.astype(BF16)
            dab_s[pl.ds(0, rows), pl.ds(ff + h * fc, fc)] = db.astype(BF16)
        for n in range(4):
            cols = pl.ds(n * nc, nc)
            o = dot(u_s[pl.ds(0, rows), :], wv[slot, pl.ds(width, ff), cols]).astype(BF16).astype(F32)
            acc[i, 0, :, cols] += jnp.where(routed, gate * o, 0.0)
            dxp = dot_nt(dab_s[pl.ds(0, rows), :], wv[slot, pl.ds(n * nc, nc), :]).astype(BF16).astype(F32)
            acc[i, 1, :, cols] += jnp.where(routed, dxp, 0.0)

    def run(copies_):
        for c in copies_:
            c.start()
        for c in copies_:
            c.wait()

    def at_steps(s, pumps):
        for k, pump in pumps.items():
            pl.when(s == k)(pump)

    def forward(name, key):
        arrived((name, key, "+"), (name, key, "-"))
        start((name, key, "2+"), (name, key, "2-"))

    def partner_weights():
        arrived(("wp", 0))
        run([stage_w(1, 1)])

    def row_neighbours():
        for name in ("g", "x", "d"):
            forward(name, 0)
        arrived(("d", "y", "+"), ("d", "y", "-"))
        start(("d", "y", "2+"), ("d", "y", "2-"))
        for j in (1, 2):
            start(("d", j, "+"), ("d", j, "-"))
        for i in (1, 2):
            share("gxd", 0, i)
        run(stage_row(1, 9) + stage_row(2, 12))
        for j in (1, 2):
            share("d", j, 0)

    def row_far():
        for name in ("g", "x", "d"):
            arrived((name, 0, "2+"), (name, 0, "2-"))
        share("gxd", 0, 3)
        run(stage_row(3, 9))

    def first_steps(s, carry):
        i, e = s // 2, lax.rem(s, 2)
        at_steps(s, {1: partner_weights, 2: row_neighbours, 6: row_far})
        row_step(e, i, 0, e)
        return carry

    lax.fori_loop(0, 8, first_steps, 0)
    for c in own_stores:
        c.wait()

    def stage_pair(j, i, slot):
        gates = gg.at[i, :, column] if j == 0 else gy.at[j, :, i]
        return [local(xg.at[j, i], xs.at[slot], 9 + slot), local(dg.at[j, i], ds.at[slot], 11 + slot),
                local(gates, gs.at[slot], 13 + slot)]

    def get_pair(j, i, slot):
        arrived(("xp", j, i), ("dp", j, i))
        if j == 0:
            arrived(("gp", 0, i))
        for c in stage_pair(j, i, slot):
            c.start()

    def grad_step(slot):
        for c in stage_pair(0, 0, slot):
            c.wait()
        gate = jnp.concatenate([gate_columns(gs[slot, p, pl.ds(2 * py + core, 1), :], nc) for p in range(2)], axis=0)
        x = xs[slot].reshape(2 * rows, width)
        routed = gate[:, :fc] > 0.0 if nc >= fc else jnp.concatenate([gate] * (fc // nc), axis=1) > 0.0
        for n in range(4):
            cols = pl.ds(n * nc, nc)
            dy = ds[slot, :, :, cols].reshape(2 * rows, nc)
            do_s[:, cols] = (gate * dy.astype(F32)).astype(BF16)
        for h in range(2):
            hidden, da, db = acts(x, do_s[...], 0, h)
            u_s[:, pl.ds(h * fc, fc)] = jnp.where(routed, hidden, 0.0).astype(BF16)
            dab_s[:, pl.ds(h * fc, fc)] = jnp.where(routed, da, 0.0).astype(BF16)
            dab_s[:, pl.ds(ff + h * fc, fc)] = jnp.where(routed, db, 0.0).astype(BF16)
        xt_s[pl.ds(0, width), :] = jnp.transpose(x)
        xt_s[pl.ds(width, ff), :] = jnp.transpose(u_s[...])
        for n in range(4):
            cols = pl.ds(n * nc, nc)
            dw[pl.ds(0, width), cols] += dot(xt_s[pl.ds(0, width), :], dab_s[:, cols])
            dw[pl.ds(width, ff), cols] += dot(xt_s[pl.ds(width, ff), :], do_s[:, cols])

    get_pair(0, 0, 0)

    def own_row_grads(q, carry):
        at_steps(q, {i - 1: functools.partial(get_pair, 0, i, i % 2) for i in range(1, 4)})
        grad_step(lax.rem(q, 2))
        return carry

    lax.fori_loop(0, 4, own_row_grads, 0)

    forward("d", 1)
    for i in (1, 2):
        share("d", 1, i)
    arrived(("w", "+"), ("w", "-"))
    start(("w", "2+"), ("w", "2-"), ("wp", 2), ("wp", 3))
    stage_w(2, 2).start()
    start(("g", "y", "+"), ("g", "y", "-"))
    for b in range(4):
        start(("x", "y", b, "+"), ("x", "y", b, "-"))
    forward("d", 2)
    for i in (1, 2):
        share("d", 2, i)

    def cotangents_far():
        arrived(("d", "y", "2+"), ("d", "y", "2-"))
        start(("d", 3, "+"), ("d", 3, "-"))
        share("d", 3, 0)

    def cotangents_last():
        forward("d", 3)
        for i in (1, 2):
            share("d", 3, i)

    def next_weights(e):
        if e == 6:
            arrived(("w", "2+"), ("w", "2-"))
            start(("wp", 6))
        elif e > 3:
            arrived(("wp", e - 2))
        stage_w(e, 2 - e % 2).start()

    def middle_steps(s, carry):
        k, i = s // 3, 3 - lax.rem(s, 3)
        slot = 2 - lax.rem(k, 2)

        @pl.when(i == 3)
        def _():
            stage_w(2, slot).wait()

        at_steps(s, {2: functools.partial(next_weights, 3), 3: cotangents_far, 5: functools.partial(next_weights, 4),
                     8: functools.partial(next_weights, 5), 10: cotangents_last, 11: functools.partial(next_weights, 6)})
        row_step(slot, i, 1 + 2 * lax.rem(k, 2), k // 2)
        return carry

    lax.fori_loop(0, 12, middle_steps, 0)
    stage_w(6, 2).wait()

    def far_weights():
        arrived(("wp", 6))
        run([stage_w(7, 1)])

    def far_sums():
        start(("r", "h+"), ("r", "h-"))
        for j in (1, 2, 3):
            arrived(("d", j, "2+"), ("d", j, "2-"))
            share("d", j, 3)

        forward("g", "y")
        for j in (1, 2):
            start(("gyp", j))

    def pass_on_x(b):
        arrived(("x", "y", b, "+"), ("x", "y", b, "-"))
        start(("x", "y", b, "2+"), ("x", "y", b, "2-"))
        share("x", 1, b)
        share("x", 2, b)

    def last_steps(s, carry):
        i, e = 3 - s // 2, lax.rem(s, 2)
        at_steps(s, {1: far_weights, 2: far_sums, 4: lambda: start(("r", "-a")), 6: lambda: start(("r", "+a")),
                     7: lambda: stage_w(2, 2).start()})
        row_step(2 - e, i, 2, e)
        return carry

    lax.fori_loop(0, 8, last_steps, 0)

    def own_steps(k, carry):
        slot = 2 - lax.rem(k, 2)
        stage_w(2, slot).wait()
        at_steps(k, {e - 3: (lambda e=e: stage_w(e, 2 - e % 2).start()) for e in (3, 4, 5)})
        row_step(slot, 0, 1 + 2 * lax.rem(k, 2), k // 2)
        return carry

    lax.fori_loop(0, 4, own_steps, 0)

    def far_x(b):
        arrived(("x", "y", b, "2+"), ("x", "y", b, "2-"))
        share("x", 3, b)

    def pass_on_sums():
        arrived(("r", "h+"), ("r", "h-"))
        acc[1, :, lo, :] += rs_half[0]
        acc[2, :, hi, :] += rs_half[1]
        start(("r", "+b"), ("r", "-b"))

    pairs = [(1 + q % 2, q // 2) for q in range(8)] + [(3, b) for b in range(4)]
    pass_on_x(0)
    arrived(("g", "y", "2+"), ("g", "y", "2-"))
    start(("gyp", 3))
    arrived(("gyp", 1), ("gyp", 2), ("gyp", 3))
    get_pair(1, 0, 0)

    def before_grad(q):
        nj, ni = pairs[q + 1]
        if nj == 2:
            get_pair(nj, ni, (q + 1) % 2)

    def after_grad(q):
        nj, ni = pairs[q + 1]
        if nj == 1:
            pass_on_x(ni)
        if nj == 3:
            far_x(ni)
        if nj != 2:
            get_pair(nj, ni, (q + 1) % 2)

    def grad_steps(q, carry):
        at_steps(q, {2: pass_on_sums})
        at_steps(q, {k: functools.partial(before_grad, k) for k in range(11)})
        grad_step(lax.rem(q, 2))
        at_steps(q, {k: functools.partial(after_grad, k) for k in range(11)})
        return carry

    lax.fori_loop(0, 12, grad_steps, 0)

    wv[1] = dw[...].astype(BF16)
    outs = [local(wv.at[1, pl.ds(0, width), pl.ds(0, ff)], dw1_out, 0),
            local(wv.at[1, pl.ds(0, width), pl.ds(ff, ff)], dw3_out, 1),
            local(wv.at[1, pl.ds(width, ff)], dw2_out, 2)]
    for c in outs:
        c.start()
    arrived(("r", "+a"), ("r", "-a"), ("r", "+b"), ("r", "-b"))
    for v, (buf, out) in enumerate(((xrow, y_out), (dyrow, dx_out))):
        buf[1] = (acc[0, v] + rs_full[0, v] + rs_full[1, v]).astype(BF16)
        c = local(buf.at[1], out, 3 + v)
        c.start()
        outs.append(c)
    for key, c in copies.items():
        c.wait_send()
    for c in outs:
        c.wait()


def copy_kernel(*refs):
    n = (len(refs) - 1) // 3
    srcs, dsts, bufs = refs[:n], refs[n:2 * n], refs[2 * n:3 * n]
    sem = refs[3 * n]
    ins = [pltpu.make_async_copy(s, b, sem.at[0, k]) for k, (s, b) in enumerate(zip(srcs, bufs))]
    outs = [pltpu.make_async_copy(b, d, sem.at[1, k]) for k, (b, d) in enumerate(zip(bufs, dsts))]
    for c in ins:
        c.start()
    for i, o in zip(ins, outs):
        i.wait()
        o.start()
    for o in outs:
        o.wait()


def solution(mesh):
    group_size = mesh.shape["ep"]
    side = math.isqrt(group_size // 2)
    tok_spec = P(("dp", "ep"), None)
    w_spec = P("ep", None, None)
    grad_spec = P(("dp", "ep"), None, None)

    def device_fn(x, ids, gates, w1, w3, w2, dy):
        rows, width = x.shape
        ff = w1.shape[2]
        experts = group_size * w1.shape[0]
        order = jnp.arange(experts, dtype=ids.dtype).reshape(side, side, 2).swapaxes(0, 1).reshape(experts)
        onehot = ids[None, :, :] == order[:, None, None]
        gate_t = jnp.sum(jnp.where(onehot, gates[None, :, :], 0.0), axis=2)
        any_spec = pl.BlockSpec(memory_space=pl.ANY)
        sds = jax.ShapeDtypeStruct
        out_shape = (
            sds((rows, width), BF16), sds((rows, width), BF16),
            sds((width, ff), BF16), sds((width, ff), BF16), sds((ff, width), BF16),
            sds((4, 4, 2, rows, width), BF16), sds((4, 4, 2, rows, width), BF16),
            sds((4, 2, experts, rows), F32), sds((4, 2, 4, 2 * side, rows), F32), sds((8, width + ff, width), BF16))
        vmem = pltpu.VMEM
        outs = pl.pallas_call(
            functools.partial(layer_kernel, side),
            out_shape=out_shape,
            in_specs=[any_spec] * 6,
            out_specs=[any_spec] * len(out_shape),
            scratch_shapes=[
                vmem((3, width + ff, width), BF16),
                vmem((4, rows, width), BF16), vmem((4, rows, width), BF16), vmem((4, experts, rows), F32),
                vmem((4, 2, rows, width), F32), vmem((2, 2, rows // 2, width), F32),
                vmem((2, 2, rows, width), F32),
                vmem((width + ff, width), F32),
                vmem((2, 2, rows, width), BF16), vmem((2, 2, rows, width), BF16), vmem((2, 2, 2 * side, rows), F32),
                vmem((2 * rows, ff), BF16), vmem((2 * rows, 2 * ff), BF16), vmem((2 * rows, width), BF16),
                vmem((width + ff, 2 * rows), BF16),
                pltpu.SemaphoreType.DMA((NUM_COPIES,)), pltpu.SemaphoreType.DMA((NUM_COPIES,)),
                pltpu.SemaphoreType.DMA((15,)),
            ],
            compiler_params=pltpu.CompilerParams(
                collective_id=0, has_side_effects=True, vmem_limit_bytes=66_900_000),
        )(x, dy, gate_t, w1[0], w3[0], w2[0])
        outs = outs[:5]
        y, dx, dw1, dw3, dw2 = pl.pallas_call(
            copy_kernel,
            out_shape=[sds(o.shape, o.dtype) for o in outs],
            in_specs=[any_spec] * 5,
            out_specs=[any_spec] * 5,
            scratch_shapes=[vmem(o.shape, o.dtype) for o in outs] + [pltpu.SemaphoreType.DMA((2, 5))],
        )(*outs)
        return y, dx, dw1[None], dw3[None], dw2[None]

    def layer_fn(tokens, expert_ids, gate_vals, w_gate, w_up, w_down, grad_out):
        return jax.shard_map(
            device_fn, mesh=mesh,
            in_specs=(tok_spec, tok_spec, tok_spec, w_spec, w_spec, w_spec, tok_spec),
            out_specs=(tok_spec, tok_spec, grad_spec, grad_spec, grad_spec), check_vma=False,
        )(tokens, expert_ids, gate_vals, w_gate, w_up, w_down, grad_out)

    return layer_fn
```

```python
import functools
import math

import jax
import jax.numpy as jnp
from jax import lax
from jax.experimental import pallas as pl
from jax.experimental.pallas import tpu as pltpu
from jax.sharding import PartitionSpec as P

MESH = pl.DeviceIdType.MESH
F32 = jnp.float32
BF16 = jnp.bfloat16
NT = (((1,), (1,)), ((), ()))
NUM_COPIES = 101


def dot(lhs, rhs):
    return jnp.dot(lhs, rhs, preferred_element_type=F32)


def dot_nt(lhs, rhs):
    return lax.dot_general(lhs, rhs, NT, preferred_element_type=F32)


def gate_columns(gate_row, width):
    cols = jnp.transpose(jnp.broadcast_to(gate_row, (128, gate_row.shape[1])))
    return jnp.concatenate([cols] * (width // 128), axis=1)


def layer_kernel(side, x_ref, dy_ref, g_ref, w1_ref, w3_ref, w2_ref,
                 y_out, dx_out, dw1_out, dw3_out, dw2_out, xg, dg, gg, gy, wg,
                 wv, xrow, dyrow, grow, acc, rs_half, rs_full, dw, xs, ds, gs, u_s, dab_s, do_s, xt_s,
                 send_sem, recv_sem, loc_sem):
    rows, width = x_ref.shape
    ff = w1_ref.shape[1]
    half = rows // 2
    fc = ff // 2
    nc = width // 4
    me = lax.axis_index("ep")
    core = lax.rem(me, 2)
    px = lax.rem(me // 2, side)
    py = me // (2 * side)

    def dev(yy, xx, cc):
        return (lax.rem(yy + side, side) * side + lax.rem(xx + side, side)) * 2 + cc

    xp, xm = dev(py, px + 1, core), dev(py, px - 1, core)
    yp, ym = dev(py + 1, px, core), dev(py - 1, px, core)
    partner = dev(py, px, 1 - core)

    copies = {}

    def reg(key, src, dst, target):
        k = len(copies)
        copies[key] = pltpu.make_async_remote_copy(
            src_ref=src, dst_ref=dst, send_sem=send_sem.at[k], recv_sem=recv_sem.at[k],
            device_id={"ep": target}, device_id_type=MESH)

    def reg_ring(key, plus, minus, src, buf, n):
        reg(key + ("+",), src, buf(2), plus)
        reg(key + ("-",), src, buf(1), minus)
        reg(key + ("2+",), buf(2).at[pl.ds(0, n // 2)], buf(3).at[pl.ds(0, n // 2)], plus)
        reg(key + ("2-",), buf(1).at[pl.ds(n // 2, n // 2)], buf(3).at[pl.ds(n // 2, n // 2)], minus)

    wn = wv.shape[1]
    reg_ring(("w",), yp, ym, wv.at[0], lambda s: wg.at[{1: 2, 2: 3, 3: 6}[s]], wn)
    reg(("wp", 0), wv.at[0], wg.at[1], partner)
    reg(("wp", 2), wg.at[2], wg.at[4], partner)
    reg(("wp", 3), wg.at[3], wg.at[5], partner)
    reg(("wp", 6), wg.at[6], wg.at[7], partner)
    column = pl.ds(pl.multiple_of(px * (2 * side), 2 * side), 2 * side)
    reg_ring(("x", 0), xp, xm, x_ref, lambda s: xg.at[0, s, 0], rows)
    reg_ring(("g", 0), xp, xm, g_ref, lambda s: gg.at[s, 0], g_ref.shape[0])
    for i in range(4):
        src = x_ref if i == 0 else xg.at[0, i, 0]
        reg_ring(("x", "y", i), yp, ym, src, lambda s, i=i: xg.at[s, i, 0], rows)
    reg_ring(("g", "y"), yp, ym, gg.at[:, 0, column], lambda s: gy.at[s, 0], 4)
    reg_ring(("d", "y"), yp, ym, dy_ref, lambda s: dg.at[s, 0, 0], rows)
    for j in range(4):
        src = dy_ref if j == 0 else dg.at[j, 0, 0]
        reg_ring(("d", j), xp, xm, src, lambda s, j=j: dg.at[j, s, 0], rows)
    for j in range(4):
        for i in range(4):
            reg(("xp", j, i), x_ref if (i, j) == (0, 0) else xg.at[j, i, 0], xg.at[j, i, 1], partner)
            reg(("dp", j, i), dy_ref if (i, j) == (0, 0) else dg.at[j, i, 0], dg.at[j, i, 1], partner)
        reg(("gp", 0, j), g_ref if j == 0 else gg.at[j, 0], gg.at[j, 1], partner)
        if j:
            reg(("gyp", j), gy.at[j, 0], gy.at[j, 1], partner)
    reg(("r", "h+"), acc.at[3, :, pl.ds(0, half)], rs_half.at[0], xp)
    reg(("r", "h-"), acc.at[3, :, pl.ds(half, half)], rs_half.at[1], xm)
    lo, hi = pl.ds(0, half), pl.ds(half, half)
    reg(("r", "+a"), acc.at[1, :, hi], rs_full.at[0, :, hi], xp)
    reg(("r", "-a"), acc.at[2, :, lo], rs_full.at[1, :, lo], xm)
    reg(("r", "+b"), acc.at[1, :, lo], rs_full.at[0, :, lo], xp)
    reg(("r", "-b"), acc.at[2, :, hi], rs_full.at[1, :, hi], xm)

    def start(*keys):
        for key in keys:
            copies[key].start()

    def arrived(*keys):
        for key in keys:
            copies[key].wait_recv()

    def share(names, j, i):
        start(*[(name + "p", j, i) for name in names])

    def local(src, dst, k):
        return pltpu.make_async_copy(src, dst, loc_sem.at[k])

    w_loads = [local(w1_ref, wv.at[0, pl.ds(0, width), pl.ds(0, ff)], 0),
               local(w3_ref, wv.at[0, pl.ds(0, width), pl.ds(ff, ff)], 1),
               local(w2_ref, wv.at[0, pl.ds(width, ff)], 2)]
    t_loads = [local(x_ref, xrow.at[0], 3), local(dy_ref, dyrow.at[0], 4), local(g_ref, grow.at[0], 5)]
    for c in w_loads + t_loads:
        c.start()

    barrier = pltpu.get_barrier_semaphore()
    for target in (xp, xm, yp, ym, partner):
        pl.semaphore_signal(barrier, inc=1, device_id={"ep": target}, device_id_type=MESH)
    pl.semaphore_wait(barrier, 5)

    start(("d", "y", "+"), ("d", "y", "-"))
    for name in ("g", "x", "d"):
        start((name, 0, "+"), (name, 0, "-"))
    for c in w_loads:
        c.wait()
    start(("w", "+"), ("w", "-"), ("wp", 0))
    share("gxd", 0, 0)
    for c in t_loads:
        c.wait()
    own_stores = [local(xrow.at[0], xg.at[0, 0, 0], 3), local(dyrow.at[0], dg.at[0, 0, 0], 4),
                  local(grow.at[0], gg.at[0, 0], 5)]
    for c in own_stores:
        c.start()
    for b in range(4):
        for v in range(2):
            acc[b, v] = jnp.zeros((rows, width), F32)
    dw[...] = jnp.zeros_like(dw)

    def stage_row(i, k):
        return [local(xg.at[0, i, 0], xrow.at[i], k), local(dg.at[0, i, 0], dyrow.at[i], k + 1),
                local(gg.at[i, 0], grow.at[i], k + 2)]

    def stage_w(e, slot):
        return local(wg.at[e], wv.at[slot], 6 + slot)

    def acts(x, do, slot, h):
        a = dot(x, wv[slot, pl.ds(0, width), pl.ds(h * fc, fc)])
        b = dot(x, wv[slot, pl.ds(0, width), pl.ds(ff + h * fc, fc)])
        du = dot_nt(do, wv[slot, pl.ds(width + h * fc, fc), :])
        sig = jax.nn.sigmoid(a)
        hidden = a * sig * b
        da = du * b * sig * (1.0 + a * (1.0 - sig))
        db = du * a * sig
        return hidden, da, db

    def row_step(slot, i, jrel, plane):
        expert = (px * side + lax.rem(py + jrel, side)) * 2 + lax.rem(core + plane, 2)
        gate = gate_columns(grow[i, pl.ds(expert, 1), :], nc)
        routed = gate > 0.0
        for n in range(4):
            cols = pl.ds(n * nc, nc)
            do_s[pl.ds(0, rows), cols] = (gate * dyrow[i, :, cols].astype(F32)).astype(BF16)
        for h in range(2):
            hidden, da, db = acts(xrow[i], do_s[pl.ds(0, rows), :], slot, h)
            u_s[pl.ds(0, rows), pl.ds(h * fc, fc)] = hidden.astype(BF16)
            dab_s[pl.ds(0, rows), pl.ds(h * fc, fc)] = da.astype(BF16)
            dab_s[pl.ds(0, rows), pl.ds(ff + h * fc, fc)] = db.astype(BF16)
        for n in range(4):
            cols = pl.ds(n * nc, nc)
            o = dot(u_s[pl.ds(0, rows), :], wv[slot, pl.ds(width, ff), cols]).astype(BF16).astype(F32)
            acc[i, 0, :, cols] += jnp.where(routed, gate * o, 0.0)
            dxp = dot_nt(dab_s[pl.ds(0, rows), :], wv[slot, pl.ds(n * nc, nc), :]).astype(BF16).astype(F32)
            acc[i, 1, :, cols] += jnp.where(routed, dxp, 0.0)

    def run(copies_):
        for c in copies_:
            c.start()
        for c in copies_:
            c.wait()

    def at_steps(s, pumps):
        for k, pump in pumps.items():
            pl.when(s == k)(pump)

    def forward(name, key):
        arrived((name, key, "+"), (name, key, "-"))
        start((name, key, "2+"), (name, key, "2-"))

    def partner_weights():
        arrived(("wp", 0))
        run([stage_w(1, 1)])

    def row_neighbours():
        for name in ("g", "x", "d"):
            forward(name, 0)
        arrived(("d", "y", "+"), ("d", "y", "-"))
        start(("d", "y", "2+"), ("d", "y", "2-"))
        for j in (1, 2):
            start(("d", j, "+"), ("d", j, "-"))
        for i in (1, 2):
            share("gxd", 0, i)
        run(stage_row(1, 9) + stage_row(2, 12))
        for j in (1, 2):
            share("d", j, 0)

    def row_far():
        for name in ("g", "x", "d"):
            arrived((name, 0, "2+"), (name, 0, "2-"))
        share("gxd", 0, 3)
        run(stage_row(3, 9))

    def first_steps(s, carry):
        i, e = s // 2, lax.rem(s, 2)
        at_steps(s, {1: partner_weights, 2: row_neighbours, 6: row_far})
        row_step(e, i, 0, e)
        return carry

    lax.fori_loop(0, 8, first_steps, 0)
    for c in own_stores:
        c.wait()
    start(("g", "y", "+"), ("g", "y", "-"))

    def stage_pair(j, i, slot):
        gates = gg.at[i, :, column] if j == 0 else gy.at[j, :, i]
        return [local(xg.at[j, i], xs.at[slot], 9 + slot), local(dg.at[j, i], ds.at[slot], 11 + slot),
                local(gates, gs.at[slot], 13 + slot)]

    def get_pair(j, i, slot):
        arrived(("xp", j, i), ("dp", j, i))
        if j == 0:
            arrived(("gp", 0, i))
        for c in stage_pair(j, i, slot):
            c.start()

    def grad_step(slot):
        for c in stage_pair(0, 0, slot):
            c.wait()
        gate = jnp.concatenate([gate_columns(gs[slot, p, pl.ds(2 * py + core, 1), :], nc) for p in range(2)], axis=0)
        x = xs[slot].reshape(2 * rows, width)
        routed = gate[:, :fc] > 0.0 if nc >= fc else jnp.concatenate([gate] * (fc // nc), axis=1) > 0.0
        for n in range(4):
            cols = pl.ds(n * nc, nc)
            dy = ds[slot, :, :, cols].reshape(2 * rows, nc)
            do_s[:, cols] = (gate * dy.astype(F32)).astype(BF16)
        for h in range(2):
            hidden, da, db = acts(x, do_s[...], 0, h)
            u_s[:, pl.ds(h * fc, fc)] = jnp.where(routed, hidden, 0.0).astype(BF16)
            dab_s[:, pl.ds(h * fc, fc)] = jnp.where(routed, da, 0.0).astype(BF16)
            dab_s[:, pl.ds(ff + h * fc, fc)] = jnp.where(routed, db, 0.0).astype(BF16)
        xt_s[pl.ds(0, width), :] = jnp.transpose(x)
        xt_s[pl.ds(width, ff), :] = jnp.transpose(u_s[...])
        for n in range(4):
            cols = pl.ds(n * nc, nc)
            dw[pl.ds(0, width), cols] += dot(xt_s[pl.ds(0, width), :], dab_s[:, cols])
            dw[pl.ds(width, ff), cols] += dot(xt_s[pl.ds(width, ff), :], do_s[:, cols])

    get_pair(0, 0, 0)

    def own_row_grads(q, carry):
        at_steps(q, {i - 1: functools.partial(get_pair, 0, i, i % 2) for i in range(1, 4)})
        grad_step(lax.rem(q, 2))
        return carry

    lax.fori_loop(0, 4, own_row_grads, 0)

    forward("d", 1)
    for i in (1, 2):
        share("d", 1, i)
    arrived(("w", "+"), ("w", "-"))
    start(("w", "2+"), ("w", "2-"), ("wp", 2), ("wp", 3))
    stage_w(2, 2).start()
    forward("d", 2)
    for i in (1, 2):
        share("d", 2, i)

    def cotangents_far():
        arrived(("d", "y", "2+"), ("d", "y", "2-"))
        start(("d", 3, "+"), ("d", 3, "-"))
        share("d", 3, 0)
        forward("g", "y")
        for j in (1, 2):
            start(("gyp", j))
        for b in range(4):
            start(("x", "y", b, "+"), ("x", "y", b, "-"))

    def cotangents_last():
        forward("d", 3)
        for i in (1, 2):
            share("d", 3, i)

    def next_weights(e):
        if e == 6:
            arrived(("w", "2+"), ("w", "2-"))
            start(("wp", 6))
        elif e > 3:
            arrived(("wp", e - 2))
        stage_w(e, 2 - e % 2).start()

    def middle_steps(s, carry):
        k, i = s // 3, 3 - lax.rem(s, 3)
        slot = 2 - lax.rem(k, 2)

        @pl.when(i == 3)
        def _():
            stage_w(2, slot).wait()

        at_steps(s, {2: functools.partial(next_weights, 3), 3: cotangents_far, 5: functools.partial(next_weights, 4),
                     8: functools.partial(next_weights, 5), 10: cotangents_last, 11: functools.partial(next_weights, 6)})
        row_step(slot, i, 1 + 2 * lax.rem(k, 2), k // 2)
        return carry

    lax.fori_loop(0, 12, middle_steps, 0)
    stage_w(6, 2).wait()

    def far_weights():
        arrived(("wp", 6))
        run([stage_w(7, 1)])

    def far_sums():
        start(("r", "h+"), ("r", "h-"))
        for j in (1, 2, 3):
            arrived(("d", j, "2+"), ("d", j, "2-"))
            share("d", j, 3)

        arrived(("g", "y", "2+"), ("g", "y", "2-"))
        start(("gyp", 3))

    def pass_on_x(b):
        arrived(("x", "y", b, "+"), ("x", "y", b, "-"))
        start(("x", "y", b, "2+"), ("x", "y", b, "2-"))
        share("x", 1, b)
        share("x", 2, b)

    def last_steps(s, carry):
        i, e = 3 - s // 2, lax.rem(s, 2)
        at_steps(s, {1: far_weights, 2: far_sums, 4: lambda: start(("r", "-a")), 6: lambda: start(("r", "+a")),
                     7: lambda: stage_w(2, 2).start()})
        row_step(2 - e, i, 2, e)
        return carry

    lax.fori_loop(0, 8, last_steps, 0)

    def own_steps(k, carry):
        slot = 2 - lax.rem(k, 2)
        stage_w(2, slot).wait()
        at_steps(k, {e - 3: (lambda e=e: stage_w(e, 2 - e % 2).start()) for e in (3, 4, 5)})
        row_step(slot, 0, 1 + 2 * lax.rem(k, 2), k // 2)
        return carry

    lax.fori_loop(0, 4, own_steps, 0)

    def far_x(b):
        arrived(("x", "y", b, "2+"), ("x", "y", b, "2-"))
        share("x", 3, b)

    def pass_on_sums():
        arrived(("r", "h+"), ("r", "h-"))
        acc[1, :, lo, :] += rs_half[0]
        acc[2, :, hi, :] += rs_half[1]
        start(("r", "+b"), ("r", "-b"))

    pairs = [(1 + q % 2, q // 2) for q in range(8)] + [(3, b) for b in range(4)]
    pass_on_x(0)
    arrived(("gyp", 1), ("gyp", 2), ("gyp", 3))
    get_pair(1, 0, 0)

    def before_grad(q):
        nj, ni = pairs[q + 1]
        if nj == 2:
            get_pair(nj, ni, (q + 1) % 2)

    def after_grad(q):
        nj, ni = pairs[q + 1]
        if nj == 1:
            pass_on_x(ni)
        if nj == 3:
            far_x(ni)
        if nj != 2:
            get_pair(nj, ni, (q + 1) % 2)

    def grad_steps(q, carry):
        at_steps(q, {2: pass_on_sums})
        at_steps(q, {k: functools.partial(before_grad, k) for k in range(11)})
        grad_step(lax.rem(q, 2))
        at_steps(q, {k: functools.partial(after_grad, k) for k in range(11)})
        return carry

    lax.fori_loop(0, 12, grad_steps, 0)

    wv[1] = dw[...].astype(BF16)
    outs = [local(wv.at[1, pl.ds(0, width), pl.ds(0, ff)], dw1_out, 0),
            local(wv.at[1, pl.ds(0, width), pl.ds(ff, ff)], dw3_out, 1),
            local(wv.at[1, pl.ds(width, ff)], dw2_out, 2)]
    for c in outs:
        c.start()
    arrived(("r", "+a"), ("r", "-a"), ("r", "+b"), ("r", "-b"))
    for v, (buf, out) in enumerate(((xrow, y_out), (dyrow, dx_out))):
        buf[1] = (acc[0, v] + rs_full[0, v] + rs_full[1, v]).astype(BF16)
        c = local(buf.at[1], out, 3 + v)
        c.start()
        outs.append(c)
    for key, c in copies.items():
        c.wait_send()
    for c in outs:
        c.wait()


def copy_kernel(*refs):
    n = (len(refs) - 1) // 3
    srcs, dsts, bufs = refs[:n], refs[n:2 * n], refs[2 * n:3 * n]
    sem = refs[3 * n]
    ins = [pltpu.make_async_copy(s, b, sem.at[0, k]) for k, (s, b) in enumerate(zip(srcs, bufs))]
    outs = [pltpu.make_async_copy(b, d, sem.at[1, k]) for k, (b, d) in enumerate(zip(bufs, dsts))]
    for c in ins:
        c.start()
    for i, o in zip(ins, outs):
        i.wait()
        o.start()
    for o in outs:
        o.wait()


def solution(mesh):
    group_size = mesh.shape["ep"]
    side = math.isqrt(group_size // 2)
    tok_spec = P(("dp", "ep"), None)
    w_spec = P("ep", None, None)
    grad_spec = P(("dp", "ep"), None, None)

    def device_fn(x, ids, gates, w1, w3, w2, dy):
        rows, width = x.shape
        ff = w1.shape[2]
        experts = group_size * w1.shape[0]
        order = jnp.arange(experts, dtype=ids.dtype).reshape(side, side, 2).swapaxes(0, 1).reshape(experts)
        onehot = ids[None, :, :] == order[:, None, None]
        gate_t = jnp.sum(jnp.where(onehot, gates[None, :, :], 0.0), axis=2)
        any_spec = pl.BlockSpec(memory_space=pl.ANY)
        sds = jax.ShapeDtypeStruct
        out_shape = (
            sds((rows, width), BF16), sds((rows, width), BF16),
            sds((width, ff), BF16), sds((width, ff), BF16), sds((ff, width), BF16),
            sds((4, 4, 2, rows, width), BF16), sds((4, 4, 2, rows, width), BF16),
            sds((4, 2, experts, rows), F32), sds((4, 2, 4, 2 * side, rows), F32), sds((8, width + ff, width), BF16))
        vmem = pltpu.VMEM
        outs = pl.pallas_call(
            functools.partial(layer_kernel, side),
            out_shape=out_shape,
            in_specs=[any_spec] * 6,
            out_specs=[any_spec] * len(out_shape),
            scratch_shapes=[
                vmem((3, width + ff, width), BF16),
                vmem((4, rows, width), BF16), vmem((4, rows, width), BF16), vmem((4, experts, rows), F32),
                vmem((4, 2, rows, width), F32), vmem((2, 2, rows // 2, width), F32),
                vmem((2, 2, rows, width), F32),
                vmem((width + ff, width), F32),
                vmem((2, 2, rows, width), BF16), vmem((2, 2, rows, width), BF16), vmem((2, 2, 2 * side, rows), F32),
                vmem((2 * rows, ff), BF16), vmem((2 * rows, 2 * ff), BF16), vmem((2 * rows, width), BF16),
                vmem((width + ff, 2 * rows), BF16),
                pltpu.SemaphoreType.DMA((NUM_COPIES,)), pltpu.SemaphoreType.DMA((NUM_COPIES,)),
                pltpu.SemaphoreType.DMA((15,)),
            ],
            compiler_params=pltpu.CompilerParams(
                collective_id=0, has_side_effects=True, vmem_limit_bytes=66_900_000),
        )(x, dy, gate_t, w1[0], w3[0], w2[0])
        outs = outs[:5]
        y, dx, dw1, dw3, dw2 = pl.pallas_call(
            copy_kernel,
            out_shape=[sds(o.shape, o.dtype) for o in outs],
            in_specs=[any_spec] * 5,
            out_specs=[any_spec] * 5,
            scratch_shapes=[vmem(o.shape, o.dtype) for o in outs] + [pltpu.SemaphoreType.DMA((2, 5))],
        )(*outs)
        return y, dx, dw1[None], dw3[None], dw2[None]

    def layer_fn(tokens, expert_ids, gate_vals, w_gate, w_up, w_down, grad_out):
        return jax.shard_map(
            device_fn, mesh=mesh,
            in_specs=(tok_spec, tok_spec, tok_spec, w_spec, w_spec, w_spec, tok_spec),
            out_specs=(tok_spec, tok_spec, grad_spec, grad_spec, grad_spec), check_vma=False,
        )(tokens, expert_ids, gate_vals, w_gate, w_up, w_down, grad_out)

    return layer_fn
```

```python
import functools
import math

import jax
import jax.numpy as jnp
from jax import lax
from jax.experimental import pallas as pl
from jax.experimental.pallas import tpu as pltpu
from jax.sharding import PartitionSpec as P

MESH = pl.DeviceIdType.MESH
F32 = jnp.float32
BF16 = jnp.bfloat16
NT = (((1,), (1,)), ((), ()))
NUM_COPIES = 101


def dot(lhs, rhs):
    return jnp.dot(lhs, rhs, preferred_element_type=F32)


def dot_nt(lhs, rhs):
    return lax.dot_general(lhs, rhs, NT, preferred_element_type=F32)


def gate_columns(gate_row, width):
    cols = jnp.transpose(jnp.broadcast_to(gate_row, (128, gate_row.shape[1])))
    return jnp.concatenate([cols] * (width // 128), axis=1)


def layer_kernel(side, x_ref, dy_ref, g_ref, w1_ref, w3_ref, w2_ref,
                 y_out, dx_out, dw1_out, dw3_out, dw2_out, xg, dg, gg, gy, wg,
                 wv, xrow, dyrow, grow, acc, rs_half, rs_full, dw, xs, ds, gs, u_s, dab_s, do_s, xt_s,
                 send_sem, recv_sem, loc_sem):
    rows, width = x_ref.shape
    ff = w1_ref.shape[1]
    half = rows // 2
    fc = ff // 2
    nc = width // 4
    me = lax.axis_index("ep")
    core = lax.rem(me, 2)
    px = lax.rem(me // 2, side)
    py = me // (2 * side)

    def dev(yy, xx, cc):
        return (lax.rem(yy + side, side) * side + lax.rem(xx + side, side)) * 2 + cc

    xp, xm = dev(py, px + 1, core), dev(py, px - 1, core)
    yp, ym = dev(py + 1, px, core), dev(py - 1, px, core)
    partner = dev(py, px, 1 - core)

    copies = {}

    def reg(key, src, dst, target):
        k = len(copies)
        copies[key] = pltpu.make_async_remote_copy(
            src_ref=src, dst_ref=dst, send_sem=send_sem.at[k], recv_sem=recv_sem.at[k],
            device_id={"ep": target}, device_id_type=MESH)

    def reg_ring(key, plus, minus, src, buf, n):
        reg(key + ("+",), src, buf(2), plus)
        reg(key + ("-",), src, buf(1), minus)
        reg(key + ("2+",), buf(2).at[pl.ds(0, n // 2)], buf(3).at[pl.ds(0, n // 2)], plus)
        reg(key + ("2-",), buf(1).at[pl.ds(n // 2, n // 2)], buf(3).at[pl.ds(n // 2, n // 2)], minus)

    wn = wv.shape[1]
    reg_ring(("w",), yp, ym, wv.at[0], lambda s: wg.at[{1: 2, 2: 3, 3: 6}[s]], wn)
    reg(("wp", 0), wv.at[0], wg.at[1], partner)
    reg(("wp", 2), wg.at[2], wg.at[4], partner)
    reg(("wp", 3), wg.at[3], wg.at[5], partner)
    reg(("wp", 6), wg.at[6], wg.at[7], partner)
    column = pl.ds(pl.multiple_of(px * (2 * side), 2 * side), 2 * side)
    reg_ring(("x", 0), xp, xm, x_ref, lambda s: xg.at[0, s, 0], rows)
    reg_ring(("g", 0), xp, xm, g_ref, lambda s: gg.at[s, 0], g_ref.shape[0])
    for i in range(4):
        src = x_ref if i == 0 else xg.at[0, i, 0]
        reg_ring(("x", "y", i), yp, ym, src, lambda s, i=i: xg.at[s, i, 0], rows)
    reg_ring(("g", "y"), yp, ym, gg.at[:, 0, column], lambda s: gy.at[s, 0], 4)
    reg_ring(("d", "y"), yp, ym, dy_ref, lambda s: dg.at[s, 0, 0], rows)
    for j in range(4):
        src = dy_ref if j == 0 else dg.at[j, 0, 0]
        reg_ring(("d", j), xp, xm, src, lambda s, j=j: dg.at[j, s, 0], rows)
    for j in range(4):
        for i in range(4):
            reg(("xp", j, i), x_ref if (i, j) == (0, 0) else xg.at[j, i, 0], xg.at[j, i, 1], partner)
            reg(("dp", j, i), dy_ref if (i, j) == (0, 0) else dg.at[j, i, 0], dg.at[j, i, 1], partner)
        reg(("gp", 0, j), g_ref if j == 0 else gg.at[j, 0], gg.at[j, 1], partner)
        if j:
            reg(("gyp", j), gy.at[j, 0], gy.at[j, 1], partner)
    reg(("r", "h+"), acc.at[3, :, pl.ds(0, half)], rs_half.at[0], xp)
    reg(("r", "h-"), acc.at[3, :, pl.ds(half, half)], rs_half.at[1], xm)
    lo, hi = pl.ds(0, half), pl.ds(half, half)
    reg(("r", "+a"), acc.at[1, :, hi], rs_full.at[0, :, hi], xp)
    reg(("r", "-a"), acc.at[2, :, lo], rs_full.at[1, :, lo], xm)
    reg(("r", "+b"), acc.at[1, :, lo], rs_full.at[0, :, lo], xp)
    reg(("r", "-b"), acc.at[2, :, hi], rs_full.at[1, :, hi], xm)

    def start(*keys):
        for key in keys:
            copies[key].start()

    def arrived(*keys):
        for key in keys:
            copies[key].wait_recv()

    def share(names, j, i):
        start(*[(name + "p", j, i) for name in names])

    def local(src, dst, k):
        return pltpu.make_async_copy(src, dst, loc_sem.at[k])

    w_loads = [local(w1_ref, wv.at[0, pl.ds(0, width), pl.ds(0, ff)], 0),
               local(w3_ref, wv.at[0, pl.ds(0, width), pl.ds(ff, ff)], 1),
               local(w2_ref, wv.at[0, pl.ds(width, ff)], 2)]
    t_loads = [local(x_ref, xrow.at[0], 3), local(dy_ref, dyrow.at[0], 4), local(g_ref, grow.at[0], 5)]
    for c in w_loads + t_loads:
        c.start()

    barrier = pltpu.get_barrier_semaphore()
    for target in (xp, xm, yp, ym, partner):
        pl.semaphore_signal(barrier, inc=1, device_id={"ep": target}, device_id_type=MESH)
    pl.semaphore_wait(barrier, 5)

    start(("d", "y", "+"), ("d", "y", "-"))
    for name in ("g", "x", "d"):
        start((name, 0, "+"), (name, 0, "-"))
    for c in w_loads:
        c.wait()
    start(("w", "+"), ("w", "-"), ("wp", 0))
    share("gxd", 0, 0)
    for c in t_loads:
        c.wait()
    own_stores = [local(xrow.at[0], xg.at[0, 0, 0], 3), local(dyrow.at[0], dg.at[0, 0, 0], 4),
                  local(grow.at[0], gg.at[0, 0], 5)]
    for c in own_stores:
        c.start()
    for b in range(4):
        for v in range(2):
            acc[b, v] = jnp.zeros((rows, width), F32)
    dw[...] = jnp.zeros_like(dw)

    def stage_row(i, k):
        return [local(xg.at[0, i, 0], xrow.at[i], k), local(dg.at[0, i, 0], dyrow.at[i], k + 1),
                local(gg.at[i, 0], grow.at[i], k + 2)]

    def stage_w(e, slot):
        return local(wg.at[e], wv.at[slot], 6 + slot)

    def acts(x, do, slot, h):
        a = dot(x, wv[slot, pl.ds(0, width), pl.ds(h * fc, fc)])
        b = dot(x, wv[slot, pl.ds(0, width), pl.ds(ff + h * fc, fc)])
        du = dot_nt(do, wv[slot, pl.ds(width + h * fc, fc), :])
        sig = jax.nn.sigmoid(a)
        hidden = a * sig * b
        da = du * b * sig * (1.0 + a * (1.0 - sig))
        db = du * a * sig
        return hidden, da, db

    def row_step(slot, i, jrel, plane):
        expert = (px * side + lax.rem(py + jrel, side)) * 2 + lax.rem(core + plane, 2)
        gate = gate_columns(grow[i, pl.ds(expert, 1), :], nc)
        routed = gate > 0.0
        for n in range(4):
            cols = pl.ds(n * nc, nc)
            do_s[pl.ds(0, rows), cols] = (gate * dyrow[i, :, cols].astype(F32)).astype(BF16)
        for h in range(2):
            hidden, da, db = acts(xrow[i], do_s[pl.ds(0, rows), :], slot, h)
            u_s[pl.ds(0, rows), pl.ds(h * fc, fc)] = hidden.astype(BF16)
            dab_s[pl.ds(0, rows), pl.ds(h * fc, fc)] = da.astype(BF16)
            dab_s[pl.ds(0, rows), pl.ds(ff + h * fc, fc)] = db.astype(BF16)
        for n in range(4):
            cols = pl.ds(n * nc, nc)
            o = dot(u_s[pl.ds(0, rows), :], wv[slot, pl.ds(width, ff), cols]).astype(BF16).astype(F32)
            acc[i, 0, :, cols] += jnp.where(routed, gate * o, 0.0)
            dxp = dot_nt(dab_s[pl.ds(0, rows), :], wv[slot, pl.ds(n * nc, nc), :]).astype(BF16).astype(F32)
            acc[i, 1, :, cols] += jnp.where(routed, dxp, 0.0)

    def run(copies_):
        for c in copies_:
            c.start()
        for c in copies_:
            c.wait()

    def at_steps(s, pumps):
        for k, pump in pumps.items():
            pl.when(s == k)(pump)

    def forward(name, key):
        arrived((name, key, "+"), (name, key, "-"))
        start((name, key, "2+"), (name, key, "2-"))

    def partner_weights():
        arrived(("wp", 0))
        run([stage_w(1, 1)])

    def row_neighbours():
        for name in ("g", "x", "d"):
            forward(name, 0)
        arrived(("d", "y", "+"), ("d", "y", "-"))
        start(("d", "y", "2+"), ("d", "y", "2-"))
        for j in (1, 2):
            start(("d", j, "+"), ("d", j, "-"))
        for i in (1, 2):
            share("gxd", 0, i)
        run(stage_row(1, 9) + stage_row(2, 12))
        for j in (1, 2):
            share("d", j, 0)

    def row_far():
        for name in ("g", "x", "d"):
            arrived((name, 0, "2+"), (name, 0, "2-"))
        share("gxd", 0, 3)
        run(stage_row(3, 9))

    def first_steps(s, carry):
        i, e = s // 2, lax.rem(s, 2)
        at_steps(s, {1: partner_weights, 2: row_neighbours, 6: row_far})
        row_step(e, i, 0, e)
        return carry

    lax.fori_loop(0, 8, first_steps, 0)
    for c in own_stores:
        c.wait()
    start(("g", "y", "+"), ("g", "y", "-"))

    def stage_pair(j, i, slot):
        gates = gg.at[i, :, column] if j == 0 else gy.at[j, :, i]
        return [local(xg.at[j, i], xs.at[slot], 9 + slot), local(dg.at[j, i], ds.at[slot], 11 + slot),
                local(gates, gs.at[slot], 13 + slot)]

    def get_pair(j, i, slot):
        arrived(("xp", j, i), ("dp", j, i))
        if j == 0:
            arrived(("gp", 0, i))
        for c in stage_pair(j, i, slot):
            c.start()

    def grad_step(slot):
        for c in stage_pair(0, 0, slot):
            c.wait()
        gate = jnp.concatenate([gate_columns(gs[slot, p, pl.ds(2 * py + core, 1), :], nc) for p in range(2)], axis=0)
        x = xs[slot].reshape(2 * rows, width)
        routed = gate[:, :fc] > 0.0 if nc >= fc else jnp.concatenate([gate] * (fc // nc), axis=1) > 0.0
        for n in range(4):
            cols = pl.ds(n * nc, nc)
            dy = ds[slot, :, :, cols].reshape(2 * rows, nc)
            do_s[:, cols] = (gate * dy.astype(F32)).astype(BF16)
        for h in range(2):
            hidden, da, db = acts(x, do_s[...], 0, h)
            u_s[:, pl.ds(h * fc, fc)] = jnp.where(routed, hidden, 0.0).astype(BF16)
            dab_s[:, pl.ds(h * fc, fc)] = jnp.where(routed, da, 0.0).astype(BF16)
            dab_s[:, pl.ds(ff + h * fc, fc)] = jnp.where(routed, db, 0.0).astype(BF16)
        xt_s[pl.ds(0, width), :] = jnp.transpose(x)
        xt_s[pl.ds(width, ff), :] = jnp.transpose(u_s[...])
        for n in range(4):
            cols = pl.ds(n * nc, nc)
            dw[pl.ds(0, width), cols] += dot(xt_s[pl.ds(0, width), :], dab_s[:, cols])
            dw[pl.ds(width, ff), cols] += dot(xt_s[pl.ds(width, ff), :], do_s[:, cols])

    get_pair(0, 0, 0)

    def own_row_grads(q, carry):
        at_steps(q, {i - 1: functools.partial(get_pair, 0, i, i % 2) for i in range(1, 4)})
        grad_step(lax.rem(q, 2))
        return carry

    lax.fori_loop(0, 4, own_row_grads, 0)

    forward("d", 1)
    for i in (1, 2):
        share("d", 1, i)
    arrived(("w", "+"), ("w", "-"))
    start(("w", "2+"), ("w", "2-"), ("wp", 2), ("wp", 3))
    stage_w(2, 2).start()
    forward("d", 2)
    for i in (1, 2):
        share("d", 2, i)

    def cotangents_far():
        arrived(("d", "y", "2+"), ("d", "y", "2-"))
        start(("d", 3, "+"), ("d", 3, "-"))
        share("d", 3, 0)
        forward("g", "y")
        for j in (1, 2):
            start(("gyp", j))
        for b in range(4):
            start(("x", "y", b, "+"), ("x", "y", b, "-"))

    def cotangents_last():
        forward("d", 3)
        for i in (1, 2):
            share("d", 3, i)

    def next_weights(e):
        if e == 6:
            arrived(("w", "2+"), ("w", "2-"))
            start(("wp", 6))
        elif e > 3:
            arrived(("wp", e - 2))
        stage_w(e, 2 - e % 2).start()

    def middle_steps(s, carry):
        tail = s // 12
        k, i = (s - tail) // 3, 3 - lax.rem(s, 3) - 3 * tail
        slot = 2 - lax.rem(k, 2)

        @pl.when(i == 3)
        def _():
            stage_w(2, slot).wait()

        at_steps(s, {2: functools.partial(next_weights, 3), 3: cotangents_far, 5: functools.partial(next_weights, 4),
                     8: functools.partial(next_weights, 5), 11: cotangents_last})
        row_step(slot, i, 1 + 2 * lax.rem(k, 2), k // 2)
        return carry

    lax.fori_loop(0, 13, middle_steps, 0)
    next_weights(6)
    stage_w(6, 2).wait()

    def far_weights():
        arrived(("wp", 6))
        run([stage_w(7, 1)])

    def far_sums():
        start(("r", "h+"), ("r", "h-"))
        for j in (1, 2, 3):
            arrived(("d", j, "2+"), ("d", j, "2-"))
            share("d", j, 3)

        arrived(("g", "y", "2+"), ("g", "y", "2-"))
        start(("gyp", 3))

    def pass_on_x(b):
        arrived(("x", "y", b, "+"), ("x", "y", b, "-"))
        start(("x", "y", b, "2+"), ("x", "y", b, "2-"))
        share("x", 1, b)
        share("x", 2, b)

    def last_steps(s, carry):
        late = s // 4
        i = (1 - late) * (3 - lax.rem(s, 2)) + late * (3 - s // 2)
        e = (1 - late) * (s // 2) + late * lax.rem(s, 2)
        at_steps(s, {2: far_weights, 3: far_sums, 4: lambda: start(("r", "-a")), 6: lambda: start(("r", "+a")),
                     7: near_x})
        row_step(2 - e, i, 2, e)
        return carry

    def near_x():
        stage_w(2, 2).start()
        pass_on_x(0)

    lax.fori_loop(0, 8, last_steps, 0)
    arrived(("gyp", 1), ("gyp", 2), ("gyp", 3))
    get_pair(1, 0, 0)

    def own_steps(k, carry):
        slot = 2 - lax.rem(k, 2)
        stage_w(2, slot).wait()
        at_steps(k, {0: lambda: stage_w(3, 1).start(), 1: lambda: stage_w(4, 2).start(), 2: lambda: pass_on_x(1)})
        row_step(slot, 0, 1 + 2 * lax.rem(k, 2), k // 2)
        return carry

    lax.fori_loop(0, 3, own_steps, 0)

    def far_x(b):
        arrived(("x", "y", b, "2+"), ("x", "y", b, "2-"))
        share("x", 3, b)

    def pass_on_sums():
        arrived(("r", "h+"), ("r", "h-"))
        acc[1, :, lo, :] += rs_half[0]
        acc[2, :, hi, :] += rs_half[1]
        start(("r", "+b"), ("r", "-b"))

    pairs = [(1 + q % 2, q // 2) for q in range(8)] + [(3, b) for b in range(4)]
    before = {3: lambda: pass_on_x(2), 5: lambda: pass_on_x(3), 7: lambda: far_x(0), 8: lambda: far_x(1),
              9: lambda: far_x(2), 10: lambda: far_x(3)}

    def before_grad(q):
        if q in before:
            before[q]()
        nj, ni = pairs[q + 1]
        if nj == 2 or (nj, ni) == (1, 1):
            get_pair(nj, ni, (q + 1) % 2)

    def after_grad(q):
        nj, ni = pairs[q + 1]
        if not (nj == 2 or (nj, ni) == (1, 1)):
            get_pair(nj, ni, (q + 1) % 2)

    def grad_steps(q, carry):
        at_steps(q, {2: pass_on_sums})
        at_steps(q, {k: functools.partial(before_grad, k) for k in range(11)})
        grad_step(lax.rem(q, 2))
        at_steps(q, {k: functools.partial(after_grad, k) for k in range(11)})
        return carry

    lax.fori_loop(0, 12, grad_steps, 0)

    wv[1] = dw[...].astype(BF16)
    outs = [local(wv.at[1, pl.ds(0, width), pl.ds(0, ff)], dw1_out, 0),
            local(wv.at[1, pl.ds(0, width), pl.ds(ff, ff)], dw3_out, 1),
            local(wv.at[1, pl.ds(width, ff)], dw2_out, 2)]
    for c in outs:
        c.start()
    arrived(("r", "+a"), ("r", "-a"), ("r", "+b"), ("r", "-b"))
    for v, (buf, out) in enumerate(((xrow, y_out), (dyrow, dx_out))):
        buf[1] = (acc[0, v] + rs_full[0, v] + rs_full[1, v]).astype(BF16)
        c = local(buf.at[1], out, 3 + v)
        c.start()
        outs.append(c)
    for key, c in copies.items():
        c.wait_send()
    for c in outs:
        c.wait()


def copy_kernel(*refs):
    n = (len(refs) - 1) // 3
    srcs, dsts, bufs = refs[:n], refs[n:2 * n], refs[2 * n:3 * n]
    sem = refs[3 * n]
    ins = [pltpu.make_async_copy(s, b, sem.at[0, k]) for k, (s, b) in enumerate(zip(srcs, bufs))]
    outs = [pltpu.make_async_copy(b, d, sem.at[1, k]) for k, (b, d) in enumerate(zip(bufs, dsts))]
    for c in ins:
        c.start()
    for i, o in zip(ins, outs):
        i.wait()
        o.start()
    for o in outs:
        o.wait()


def solution(mesh):
    group_size = mesh.shape["ep"]
    side = math.isqrt(group_size // 2)
    tok_spec = P(("dp", "ep"), None)
    w_spec = P("ep", None, None)
    grad_spec = P(("dp", "ep"), None, None)

    def device_fn(x, ids, gates, w1, w3, w2, dy):
        rows, width = x.shape
        ff = w1.shape[2]
        experts = group_size * w1.shape[0]
        order = jnp.arange(experts, dtype=ids.dtype).reshape(side, side, 2).swapaxes(0, 1).reshape(experts)
        onehot = ids[None, :, :] == order[:, None, None]
        gate_t = jnp.sum(jnp.where(onehot, gates[None, :, :], 0.0), axis=2)
        any_spec = pl.BlockSpec(memory_space=pl.ANY)
        sds = jax.ShapeDtypeStruct
        out_shape = (
            sds((rows, width), BF16), sds((rows, width), BF16),
            sds((width, ff), BF16), sds((width, ff), BF16), sds((ff, width), BF16),
            sds((4, 4, 2, rows, width), BF16), sds((4, 4, 2, rows, width), BF16),
            sds((4, 2, experts, rows), F32), sds((4, 2, 4, 2 * side, rows), F32), sds((8, width + ff, width), BF16))
        vmem = pltpu.VMEM
        outs = pl.pallas_call(
            functools.partial(layer_kernel, side),
            out_shape=out_shape,
            in_specs=[any_spec] * 6,
            out_specs=[any_spec] * len(out_shape),
            scratch_shapes=[
                vmem((3, width + ff, width), BF16),
                vmem((4, rows, width), BF16), vmem((4, rows, width), BF16), vmem((4, experts, rows), F32),
                vmem((4, 2, rows, width), F32), vmem((2, 2, rows // 2, width), F32),
                vmem((2, 2, rows, width), F32),
                vmem((width + ff, width), F32),
                vmem((2, 2, rows, width), BF16), vmem((2, 2, rows, width), BF16), vmem((2, 2, 2 * side, rows), F32),
                vmem((2 * rows, ff), BF16), vmem((2 * rows, 2 * ff), BF16), vmem((2 * rows, width), BF16),
                vmem((width + ff, 2 * rows), BF16),
                pltpu.SemaphoreType.DMA((NUM_COPIES,)), pltpu.SemaphoreType.DMA((NUM_COPIES,)),
                pltpu.SemaphoreType.DMA((15,)),
            ],
            compiler_params=pltpu.CompilerParams(
                collective_id=0, has_side_effects=True, vmem_limit_bytes=66_900_000),
        )(x, dy, gate_t, w1[0], w3[0], w2[0])
        outs = outs[:5]
        y, dx, dw1, dw3, dw2 = pl.pallas_call(
            copy_kernel,
            out_shape=[sds(o.shape, o.dtype) for o in outs],
            in_specs=[any_spec] * 5,
            out_specs=[any_spec] * 5,
            scratch_shapes=[vmem(o.shape, o.dtype) for o in outs] + [pltpu.SemaphoreType.DMA((2, 5))],
        )(*outs)
        return y, dx, dw1[None], dw3[None], dw2[None]

    def layer_fn(tokens, expert_ids, gate_vals, w_gate, w_up, w_down, grad_out):
        return jax.shard_map(
            device_fn, mesh=mesh,
            in_specs=(tok_spec, tok_spec, tok_spec, w_spec, w_spec, w_spec, tok_spec),
            out_specs=(tok_spec, tok_spec, grad_spec, grad_spec, grad_spec), check_vma=False,
        )(tokens, expert_ids, gate_vals, w_gate, w_up, w_down, grad_out)

    return layer_fn
```

```python
import functools
import math

import jax
import jax.numpy as jnp
from jax import lax
from jax.experimental import pallas as pl
from jax.experimental.pallas import tpu as pltpu
from jax.sharding import PartitionSpec as P

MESH = pl.DeviceIdType.MESH
F32 = jnp.float32
BF16 = jnp.bfloat16
NT = (((1,), (1,)), ((), ()))
NUM_COPIES = 101


def dot(lhs, rhs):
    return jnp.dot(lhs, rhs, preferred_element_type=F32)


def dot_nt(lhs, rhs):
    return lax.dot_general(lhs, rhs, NT, preferred_element_type=F32)


def gate_columns(gate_row, width):
    cols = jnp.transpose(jnp.broadcast_to(gate_row, (128, gate_row.shape[1])))
    return jnp.concatenate([cols] * (width // 128), axis=1)


def layer_kernel(side, x_ref, dy_ref, g_ref, w1_ref, w3_ref, w2_ref,
                 y_out, dx_out, dw1_out, dw3_out, dw2_out, xg, dg, gg, gy, wg,
                 wv, xrow, dyrow, grow, acc, rs_half, rs_full, dw, xs, ds, gs, u_s, dab_s, do_s, xt_s,
                 send_sem, recv_sem, loc_sem):
    rows, width = x_ref.shape
    ff = w1_ref.shape[1]
    half = rows // 2
    fc = ff // 2
    nc = width // 4
    me = lax.axis_index("ep")
    core = lax.rem(me, 2)
    px = lax.rem(me // 2, side)
    py = me // (2 * side)

    def dev(yy, xx, cc):
        return (lax.rem(yy + side, side) * side + lax.rem(xx + side, side)) * 2 + cc

    xp, xm = dev(py, px + 1, core), dev(py, px - 1, core)
    yp, ym = dev(py + 1, px, core), dev(py - 1, px, core)
    partner = dev(py, px, 1 - core)

    copies = {}

    def reg(key, src, dst, target):
        k = len(copies)
        copies[key] = pltpu.make_async_remote_copy(
            src_ref=src, dst_ref=dst, send_sem=send_sem.at[k], recv_sem=recv_sem.at[k],
            device_id={"ep": target}, device_id_type=MESH)

    def reg_ring(key, plus, minus, src, buf, n):
        reg(key + ("+",), src, buf(2), plus)
        reg(key + ("-",), src, buf(1), minus)
        reg(key + ("2+",), buf(2).at[pl.ds(0, n // 2)], buf(3).at[pl.ds(0, n // 2)], plus)
        reg(key + ("2-",), buf(1).at[pl.ds(n // 2, n // 2)], buf(3).at[pl.ds(n // 2, n // 2)], minus)

    wn = wv.shape[1]
    reg_ring(("w",), yp, ym, wv.at[0], lambda s: wg.at[{1: 2, 2: 3, 3: 6}[s]], wn)
    reg(("wp", 0), wv.at[0], wg.at[1], partner)
    reg(("wp", 2), wg.at[2], wg.at[4], partner)
    reg(("wp", 3), wg.at[3], wg.at[5], partner)
    reg(("wp", 6), wg.at[6], wv.at[3], partner)
    column = pl.ds(pl.multiple_of(px * (2 * side), 2 * side), 2 * side)
    reg_ring(("x", 0), xp, xm, x_ref, lambda s: xg.at[0, s, 0], rows)
    reg_ring(("g", 0), xp, xm, g_ref, lambda s: gg.at[s, 0], g_ref.shape[0])
    for i in range(4):
        src = x_ref if i == 0 else xg.at[0, i, 0]
        reg_ring(("x", "y", i), yp, ym, src, lambda s, i=i: xg.at[s, i, 0], rows)
    reg_ring(("g", "y"), yp, ym, gg.at[:, 0, column], lambda s: gy.at[s, 0], 4)
    reg_ring(("d", "y"), yp, ym, dy_ref, lambda s: dg.at[s, 0, 0], rows)
    for j in range(4):
        src = dy_ref if j == 0 else dg.at[j, 0, 0]
        reg_ring(("d", j), xp, xm, src, lambda s, j=j: dg.at[j, s, 0], rows)
    for j in range(4):
        for i in range(4):
            reg(("xp", j, i), x_ref if (i, j) == (0, 0) else xg.at[j, i, 0], xg.at[j, i, 1], partner)
            reg(("dp", j, i), dy_ref if (i, j) == (0, 0) else dg.at[j, i, 0], dg.at[j, i, 1], partner)
        reg(("gp", 0, j), g_ref if j == 0 else gg.at[j, 0], gg.at[j, 1], partner)
        if j:
            reg(("gyp", j), gy.at[j, 0], gy.at[j, 1], partner)
    reg(("r", "h+"), acc.at[3, :, pl.ds(0, half)], rs_half.at[0], xp)
    reg(("r", "h-"), acc.at[3, :, pl.ds(half, half)], rs_half.at[1], xm)
    lo, hi = pl.ds(0, half), pl.ds(half, half)
    reg(("r", "+a"), acc.at[1, :, hi], rs_full.at[0, :, hi], xp)
    reg(("r", "-a"), acc.at[2, :, lo], rs_full.at[1, :, lo], xm)
    reg(("r", "+b"), acc.at[1, :, lo], rs_full.at[0, :, lo], xp)
    reg(("r", "-b"), acc.at[2, :, hi], rs_full.at[1, :, hi], xm)

    def start(*keys):
        for key in keys:
            copies[key].start()

    def arrived(*keys):
        for key in keys:
            copies[key].wait_recv()

    def share(names, j, i):
        start(*[(name + "p", j, i) for name in names])

    def local(src, dst, k):
        return pltpu.make_async_copy(src, dst, loc_sem.at[k])

    w_loads = [local(w1_ref, wv.at[0, pl.ds(0, width), pl.ds(0, ff)], 0),
               local(w3_ref, wv.at[0, pl.ds(0, width), pl.ds(ff, ff)], 1),
               local(w2_ref, wv.at[0, pl.ds(width, ff)], 2)]
    t_loads = [local(x_ref, xrow.at[0], 3), local(dy_ref, dyrow.at[0], 4), local(g_ref, grow.at[0], 5)]
    for c in w_loads + t_loads:
        c.start()

    barrier = pltpu.get_barrier_semaphore()
    for target in (xp, xm, yp, ym, partner):
        pl.semaphore_signal(barrier, inc=1, device_id={"ep": target}, device_id_type=MESH)
    pl.semaphore_wait(barrier, 5)

    start(("d", "y", "+"), ("d", "y", "-"))
    for name in ("g", "x", "d"):
        start((name, 0, "+"), (name, 0, "-"))
    for c in w_loads:
        c.wait()
    start(("w", "+"), ("w", "-"), ("wp", 0))
    share("gxd", 0, 0)
    for c in t_loads:
        c.wait()
    own_stores = [local(xrow.at[0], xg.at[0, 0, 0], 3), local(dyrow.at[0], dg.at[0, 0, 0], 4),
                  local(grow.at[0], gg.at[0, 0], 5)]
    for c in own_stores:
        c.start()
    for b in range(4):
        for v in range(2):
            acc[b, v] = jnp.zeros((rows, width), F32)
    dw[...] = jnp.zeros_like(dw)

    def stage_row(i, k):
        return [local(xg.at[0, i, 0], xrow.at[i], k), local(dg.at[0, i, 0], dyrow.at[i], k + 1),
                local(gg.at[i, 0], grow.at[i], k + 2)]

    def stage_w(e, slot):
        return local(wg.at[e], wv.at[slot], 6 + slot)

    def acts(x, do, slot, h):
        a = dot(x, wv[slot, pl.ds(0, width), pl.ds(h * fc, fc)])
        b = dot(x, wv[slot, pl.ds(0, width), pl.ds(ff + h * fc, fc)])
        du = dot_nt(do, wv[slot, pl.ds(width + h * fc, fc), :])
        sig = jax.nn.sigmoid(a)
        hidden = a * sig * b
        da = du * b * sig * (1.0 + a * (1.0 - sig))
        db = du * a * sig
        return hidden, da, db

    def row_step(slot, i, jrel, plane):
        expert = (px * side + lax.rem(py + jrel, side)) * 2 + lax.rem(core + plane, 2)
        gate = gate_columns(grow[i, pl.ds(expert, 1), :], nc)
        routed = gate > 0.0
        for n in range(4):
            cols = pl.ds(n * nc, nc)
            do_s[pl.ds(0, rows), cols] = (gate * dyrow[i, :, cols].astype(F32)).astype(BF16)
        for h in range(2):
            hidden, da, db = acts(xrow[i], do_s[pl.ds(0, rows), :], slot, h)
            u_s[pl.ds(0, rows), pl.ds(h * fc, fc)] = hidden.astype(BF16)
            dab_s[pl.ds(0, rows), pl.ds(h * fc, fc)] = da.astype(BF16)
            dab_s[pl.ds(0, rows), pl.ds(ff + h * fc, fc)] = db.astype(BF16)
        for n in range(4):
            cols = pl.ds(n * nc, nc)
            o = dot(u_s[pl.ds(0, rows), :], wv[slot, pl.ds(width, ff), cols]).astype(BF16).astype(F32)
            acc[i, 0, :, cols] += jnp.where(routed, gate * o, 0.0)
            dxp = dot_nt(dab_s[pl.ds(0, rows), :], wv[slot, pl.ds(n * nc, nc), :]).astype(BF16).astype(F32)
            acc[i, 1, :, cols] += jnp.where(routed, dxp, 0.0)

    def run(copies_):
        for c in copies_:
            c.start()
        for c in copies_:
            c.wait()

    def at_steps(s, pumps):
        for k, pump in pumps.items():
            pl.when(s == k)(pump)

    def forward(name, key):
        arrived((name, key, "+"), (name, key, "-"))
        start((name, key, "2+"), (name, key, "2-"))

    def partner_weights():
        arrived(("wp", 0))
        run([stage_w(1, 1)])

    def row_neighbours():
        for name in ("g", "x", "d"):
            forward(name, 0)
        arrived(("d", "y", "+"), ("d", "y", "-"))
        start(("d", "y", "2+"), ("d", "y", "2-"))
        for j in (1, 2):
            start(("d", j, "+"), ("d", j, "-"))
        for i in (1, 2):
            share("gxd", 0, i)
        run(stage_row(1, 9) + stage_row(2, 12))
        for j in (1, 2):
            share("d", j, 0)

    def row_far():
        for name in ("g", "x", "d"):
            arrived((name, 0, "2+"), (name, 0, "2-"))
        share("gxd", 0, 3)
        run(stage_row(3, 9))

    def first_steps(s, carry):
        i, e = s // 2, lax.rem(s, 2)
        at_steps(s, {1: partner_weights, 2: row_neighbours, 6: row_far})
        row_step(e, i, 0, e)
        return carry

    lax.fori_loop(0, 8, first_steps, 0)
    for c in own_stores:
        c.wait()
    start(("g", "y", "+"), ("g", "y", "-"))

    def stage_pair(j, i, slot):
        gates = gg.at[i, :, column] if j == 0 else gy.at[j, :, i]
        return [local(xg.at[j, i], xs.at[slot], 9 + slot), local(dg.at[j, i], ds.at[slot], 11 + slot),
                local(gates, gs.at[slot], 13 + slot)]

    def get_pair(j, i, slot):
        arrived(("xp", j, i), ("dp", j, i))
        if j == 0:
            arrived(("gp", 0, i))
        for c in stage_pair(j, i, slot):
            c.start()

    def grad_step(slot, between):
        for c in stage_pair(0, 0, slot):
            c.wait()
        gate = jnp.concatenate([gate_columns(gs[slot, p, pl.ds(2 * py + core, 1), :], nc) for p in range(2)], axis=0)
        x = xs[slot].reshape(2 * rows, width)
        routed = gate[:, :fc] > 0.0 if nc >= fc else jnp.concatenate([gate] * (fc // nc), axis=1) > 0.0
        for n in range(4):
            cols = pl.ds(n * nc, nc)
            dy = ds[slot, :, :, cols].reshape(2 * rows, nc)
            do_s[:, cols] = (gate * dy.astype(F32)).astype(BF16)
        for h in range(2):
            hidden, da, db = acts(x, do_s[...], 0, h)
            u_s[:, pl.ds(h * fc, fc)] = jnp.where(routed, hidden, 0.0).astype(BF16)
            dab_s[:, pl.ds(h * fc, fc)] = jnp.where(routed, da, 0.0).astype(BF16)
            dab_s[:, pl.ds(ff + h * fc, fc)] = jnp.where(routed, db, 0.0).astype(BF16)
        between()
        xt_s[pl.ds(0, width), :] = jnp.transpose(x)
        xt_s[pl.ds(width, ff), :] = jnp.transpose(u_s[...])
        for n in range(4):
            cols = pl.ds(n * nc, nc)
            dw[pl.ds(0, width), cols] += dot(xt_s[pl.ds(0, width), :], dab_s[:, cols])
            dw[pl.ds(width, ff), cols] += dot(xt_s[pl.ds(width, ff), :], do_s[:, cols])

    get_pair(0, 0, 0)

    def own_row_grads(q, carry):
        at_steps(q, {i - 1: functools.partial(get_pair, 0, i, i % 2) for i in range(1, 4)})
        grad_step(lax.rem(q, 2), lambda: None)
        return carry

    lax.fori_loop(0, 4, own_row_grads, 0)

    forward("d", 1)
    for i in (1, 2):
        share("d", 1, i)
    arrived(("w", "+"), ("w", "-"))
    start(("w", "2+"), ("w", "2-"), ("wp", 2), ("wp", 3))
    stage_w(2, 2).start()
    forward("d", 2)
    for i in (1, 2):
        share("d", 2, i)

    def cotangents_far():
        arrived(("d", "y", "2+"), ("d", "y", "2-"))
        start(("d", 3, "+"), ("d", 3, "-"))
        share("d", 3, 0)
        forward("g", "y")
        for j in (1, 2):
            start(("gyp", j))
        for b in range(4):
            start(("x", "y", b, "+"), ("x", "y", b, "-"))

    def cotangents_last():
        forward("d", 3)
        for i in (1, 2):
            share("d", 3, i)

    def next_weights(e):
        if e == 6:
            arrived(("w", "2+"), ("w", "2-"))
            start(("wp", 6))
        elif e > 3:
            arrived(("wp", e - 2))
        stage_w(e, 2 - e % 2).start()

    def middle_steps(s, carry):
        tail = s // 12
        k, i = (s - tail) // 3, 3 - lax.rem(s, 3) - 3 * tail
        slot = 2 - lax.rem(k, 2)

        @pl.when(i == 3)
        def _():
            stage_w(2, slot).wait()

        at_steps(s, {2: functools.partial(next_weights, 3), 3: cotangents_far, 5: functools.partial(next_weights, 4),
                     8: functools.partial(next_weights, 5), 11: cotangents_last})
        row_step(slot, i, 1 + 2 * lax.rem(k, 2), k // 2)
        return carry

    lax.fori_loop(0, 13, middle_steps, 0)
    next_weights(6)
    stage_w(6, 2).wait()

    def far_weights():
        arrived(("wp", 6))

    def far_sums():
        start(("r", "h+"), ("r", "h-"))
        for j in (1, 2, 3):
            arrived(("d", j, "2+"), ("d", j, "2-"))
            share("d", j, 3)

        arrived(("g", "y", "2+"), ("g", "y", "2-"))
        start(("gyp", 3))

    def pass_on_x(b):
        arrived(("x", "y", b, "+"), ("x", "y", b, "-"))
        start(("x", "y", b, "2+"), ("x", "y", b, "2-"))
        share("x", 1, b)
        share("x", 2, b)

    def last_steps(s, carry):
        late = s // 4
        i = (1 - late) * (3 - lax.rem(s, 2)) + late * (3 - s // 2)
        e = (1 - late) * (s // 2) + late * lax.rem(s, 2)
        at_steps(s, {2: far_weights, 3: far_sums, 4: lambda: start(("r", "-a")), 6: lambda: start(("r", "+a")),
                     7: near_x})
        row_step(2 + e, i, 2, e)
        return carry

    def near_x():
        stage_w(2, 2).start()
        pass_on_x(0)

    lax.fori_loop(0, 8, last_steps, 0)
    arrived(("gyp", 1), ("gyp", 2), ("gyp", 3))
    get_pair(1, 0, 0)

    def own_steps(k, carry):
        slot = 2 - lax.rem(k, 2)
        stage_w(2, slot).wait()
        at_steps(k, {0: lambda: stage_w(3, 1).start(), 1: lambda: stage_w(4, 2).start(), 2: lambda: pass_on_x(1)})
        row_step(slot, 0, 1 + 2 * lax.rem(k, 2), k // 2)
        return carry

    lax.fori_loop(0, 3, own_steps, 0)

    def far_x(b):
        arrived(("x", "y", b, "2+"), ("x", "y", b, "2-"))
        share("x", 3, b)

    def pass_on_sums():
        arrived(("r", "h+"), ("r", "h-"))
        acc[1, :, lo, :] += rs_half[0]
        acc[2, :, hi, :] += rs_half[1]
        start(("r", "+b"), ("r", "-b"))

    pairs = [(1 + q % 2, q // 2) for q in range(8)] + [(3, b) for b in range(4)]
    before = {3: lambda: pass_on_x(2), 5: lambda: pass_on_x(3), 7: lambda: far_x(0), 8: lambda: far_x(1),
              9: lambda: far_x(2), 10: lambda: far_x(3)}

    def before_grad(q):
        if q in before:
            before[q]()
        nj, ni = pairs[q + 1]
        if nj == 2 or (nj, ni) == (1, 1):
            get_pair(nj, ni, (q + 1) % 2)

    def mid_grad(q):
        nj, ni = pairs[q + 1]
        if not (nj == 2 or (nj, ni) == (1, 1)):
            get_pair(nj, ni, (q + 1) % 2)

    def grad_steps(q, carry):
        at_steps(q, {2: pass_on_sums})
        at_steps(q, {k: functools.partial(before_grad, k) for k in range(11)})
        grad_step(lax.rem(q, 2), lambda: at_steps(q, {k: functools.partial(mid_grad, k) for k in range(11)}))
        return carry

    lax.fori_loop(0, 12, grad_steps, 0)

    wv[1] = dw[...].astype(BF16)
    outs = [local(wv.at[1, pl.ds(0, width), pl.ds(0, ff)], dw1_out, 0),
            local(wv.at[1, pl.ds(0, width), pl.ds(ff, ff)], dw3_out, 1),
            local(wv.at[1, pl.ds(width, ff)], dw2_out, 2)]
    for c in outs:
        c.start()
    arrived(("r", "+a"), ("r", "-a"), ("r", "+b"), ("r", "-b"))
    for v, (buf, out) in enumerate(((xrow, y_out), (dyrow, dx_out))):
        buf[1] = (acc[0, v] + rs_full[0, v] + rs_full[1, v]).astype(BF16)
        c = local(buf.at[1], out, 3 + v)
        c.start()
        outs.append(c)
    for key, c in copies.items():
        c.wait_send()
    for c in outs:
        c.wait()


def copy_kernel(*refs):
    n = (len(refs) - 1) // 3
    srcs, dsts, bufs = refs[:n], refs[n:2 * n], refs[2 * n:3 * n]
    sem = refs[3 * n]
    ins = [pltpu.make_async_copy(s, b, sem.at[0, k]) for k, (s, b) in enumerate(zip(srcs, bufs))]
    outs = [pltpu.make_async_copy(b, d, sem.at[1, k]) for k, (b, d) in enumerate(zip(bufs, dsts))]
    for c in ins:
        c.start()
    for i, o in zip(ins, outs):
        i.wait()
        o.start()
    for o in outs:
        o.wait()


def solution(mesh):
    group_size = mesh.shape["ep"]
    side = math.isqrt(group_size // 2)
    tok_spec = P(("dp", "ep"), None)
    w_spec = P("ep", None, None)
    grad_spec = P(("dp", "ep"), None, None)

    def device_fn(x, ids, gates, w1, w3, w2, dy):
        rows, width = x.shape
        ff = w1.shape[2]
        experts = group_size * w1.shape[0]
        order = jnp.arange(experts, dtype=ids.dtype).reshape(side, side, 2).swapaxes(0, 1).reshape(experts)
        onehot = ids[None, :, :] == order[:, None, None]
        gate_t = jnp.sum(jnp.where(onehot, gates[None, :, :], 0.0), axis=2)
        any_spec = pl.BlockSpec(memory_space=pl.ANY)
        sds = jax.ShapeDtypeStruct
        out_shape = (
            sds((rows, width), BF16), sds((rows, width), BF16),
            sds((width, ff), BF16), sds((width, ff), BF16), sds((ff, width), BF16),
            sds((4, 4, 2, rows, width), BF16), sds((4, 4, 2, rows, width), BF16),
            sds((4, 2, experts, rows), F32), sds((4, 2, 4, 2 * side, rows), F32), sds((7, width + ff, width), BF16))
        vmem = pltpu.VMEM
        outs = pl.pallas_call(
            functools.partial(layer_kernel, side),
            out_shape=out_shape,
            in_specs=[any_spec] * 6,
            out_specs=[any_spec] * len(out_shape),
            scratch_shapes=[
                vmem((4, width + ff, width), BF16),
                vmem((4, rows, width), BF16), vmem((4, rows, width), BF16), vmem((4, experts, rows), F32),
                vmem((4, 2, rows, width), F32), vmem((2, 2, rows // 2, width), F32),
                vmem((2, 2, rows, width), F32),
                vmem((width + ff, width), F32),
                vmem((2, 2, rows, width), BF16), vmem((2, 2, rows, width), BF16), vmem((2, 2, 2 * side, rows), F32),
                vmem((2 * rows, ff), BF16), vmem((2 * rows, 2 * ff), BF16), vmem((2 * rows, width), BF16),
                vmem((width + ff, 2 * rows), BF16),
                pltpu.SemaphoreType.DMA((NUM_COPIES,)), pltpu.SemaphoreType.DMA((NUM_COPIES,)),
                pltpu.SemaphoreType.DMA((15,)),
            ],
            compiler_params=pltpu.CompilerParams(
                collective_id=0, has_side_effects=True, vmem_limit_bytes=66_900_000),
        )(x, dy, gate_t, w1[0], w3[0], w2[0])
        outs = outs[:5]
        y, dx, dw1, dw3, dw2 = pl.pallas_call(
            copy_kernel,
            out_shape=[sds(o.shape, o.dtype) for o in outs],
            in_specs=[any_spec] * 5,
            out_specs=[any_spec] * 5,
            scratch_shapes=[vmem(o.shape, o.dtype) for o in outs] + [pltpu.SemaphoreType.DMA((2, 5))],
        )(*outs)
        return y, dx, dw1[None], dw3[None], dw2[None]

    def layer_fn(tokens, expert_ids, gate_vals, w_gate, w_up, w_down, grad_out):
        return jax.shard_map(
            device_fn, mesh=mesh,
            in_specs=(tok_spec, tok_spec, tok_spec, w_spec, w_spec, w_spec, tok_spec),
            out_specs=(tok_spec, tok_spec, grad_spec, grad_spec, grad_spec), check_vma=False,
        )(tokens, expert_ids, gate_vals, w_gate, w_up, w_down, grad_out)

    return layer_fn
```
